32 devices in a mesh: replica: 4 (over x, core), shard: 8 (over z, y).
Axes of the slice: x: 2, y: 2, z: 4, core: 2. Of those that a mesh axis runs over, the one named last changes fastest.
Arguments:
- tokens: bfloat16 [8, 1024, 768], P('replica', 'shard'), may hold values from -6 to 6
- gain_one: bfloat16 [2, 768], P(None, 'shard'), may hold values from 0.099609375 to 1.8984375
- shift_one: bfloat16 [2, 768], P(None, 'shard'), may hold values from -4 to 4
- query_key_value_weight: bfloat16 [2, 768, 2304], P(None, 'shard'), may hold values from -0.21875 to 0.21875
- b_query: bfloat16 [2, 768], P(None, 'shard'), may hold values from -4 to 4
- b_value: bfloat16 [2, 768], P(None, 'shard'), may hold values from -4 to 4
- output_weight: bfloat16 [2, 768, 768], P(None, 'shard'), may hold values from -3.5 to 3.5
- output_proj_bias: bfloat16 [2, 768], P(None, 'shard'), may hold values from -4 to 4
- gain_two: bfloat16 [2, 768], P(None, 'shard'), may hold values from 0.099609375 to 1.8984375
- shift_two: bfloat16 [2, 768], P(None, 'shard'), may hold values from -4 to 4
- up_weight: bfloat16 [2, 768, 3072], P(None, 'shard'), may hold values from -0.21875 to 0.21875
- up_bias: bfloat16 [2, 3072], P(None, 'shard'), may hold values from -4 to 4
- down_weight: bfloat16 [2, 3072, 768], P(None, 'shard'), may hold values from -0.109375 to 0.109375
- down_bias: bfloat16 [2, 768], P(None, 'shard'), may hold values from -4 to 4
- cotangent: bfloat16 [8, 1024, 768], P('replica', 'shard'), may hold values from -6 to 6
Outputs:
- output: bfloat16 [8, 1024, 768], P('replica', 'shard')
- grad_tokens: float32 [8, 1024, 768], P('replica', 'shard')
- grad_gain_one: float32 [2, 768], P(None, 'shard')
- grad_shift_one: float32 [2, 768], P(None, 'shard')
- query_key_value_gradient: float32 [2, 768, 2304], P(None, 'shard')
- grad_b_query: float32 [2, 768], P(None, 'shard')
- grad_b_value: float32 [2, 768], P(None, 'shard')
- output_weight_gradient: float32 [2, 768, 768], P(None, 'shard')
- grad_b_out: float32 [2, 768], P(None, 'shard')
- grad_gain_two: float32 [2, 768], P(None, 'shard')
- grad_shift_two: float32 [2, 768], P(None, 'shard')
- up_weight_gradient: float32 [2, 768, 3072], P(None, 'shard')
- grad_b_up: float32 [2, 3072], P(None, 'shard')
- down_weight_gradient: float32 [2, 3072, 768], P(None, 'shard')
- grad_b_down: float32 [2, 768], P(None, 'shard')
The draws below stay inside these ranges and needn't reach their ends.
All inputs are finite; a program needn't handle non-finite values.
Results may differ from the reference program's by a relative error of at most 0.015.
The reference program's roundings to bfloat16 on the way count: a program that leaves them out, or rounds other values in their place, can miss the bound.
Values may be sent and summed in bfloat16 or wider, within the bound.
A program may use at most 256 MiB of HBM per device.

```python
import jax
import jax.numpy as jnp
from jax import lax

D = 768
HEADS = 12
HEAD_DIM = 64
FF = 3072
LENGTH = 1024
LAYERS = 2
SEQS = 8


def shard_levels(stream_key, shape, split, least, largest):
    level, own = 1.0, jax.random.fold_in(stream_key, 6)
    for axis_at, blocks in split:
        draws = jnp.exp(jax.random.uniform(jax.random.fold_in(own, axis_at), (blocks,), jnp.float32, least / len(split), largest / len(split)))
        level = level * jnp.repeat(draws, shape[axis_at] // blocks).reshape([-1 if axis == axis_at else 1 for axis in range(len(shape))])
    return level


def centred(stream_key, shape, scale, limit, shards=(), dtype=jnp.bfloat16):
    values = scale * jax.random.normal(stream_key, shape, jnp.float32)
    if shards:
        values = values * shard_levels(stream_key, shape, shards, -0.22, 0.18)
    return jnp.clip(values, -limit, limit).astype(dtype)


def setup_inputs(seed: int = 0) -> dict:
    splits = jax.random.split(jax.random.key(seed), 16)
    return {
        "tokens": centred(splits[0], (SEQS, LENGTH, D), 1.0, 6.0, ((0, 4), (1, 8))),
        "gain_one": jnp.clip(1.0 + 0.18 * jax.random.normal(splits[1], (LAYERS, D), jnp.float32), 0.099609375, 1.8984375).astype(jnp.bfloat16),
        "shift_one": centred(splits[2], (LAYERS, D), 1.0, 4.0, ((1, 8),)),
        "query_key_value_weight": centred(splits[3], (LAYERS, D, 3 * D), D ** -0.5, 0.21875, ((1, 8),)),
        "b_query": centred(splits[4], (LAYERS, D), 1.0, 4.0, ((1, 8),)),
        "b_value": centred(splits[5], (LAYERS, D), 1.0, 4.0, ((1, 8),)),
        "output_weight": centred(splits[6], (LAYERS, D, D), (max(D // 256, 1)) ** -0.5, 3.5, ((1, 8),)),
        "output_proj_bias": centred(splits[7], (LAYERS, D), 1.0, 4.0, ((1, 8),)),
        "gain_two": jnp.clip(1.0 + 0.18 * jax.random.normal(splits[8], (LAYERS, D), jnp.float32), 0.099609375, 1.8984375).astype(jnp.bfloat16),
        "shift_two": centred(splits[9], (LAYERS, D), 1.0, 4.0, ((1, 8),)),
        "up_weight": centred(splits[10], (LAYERS, D, FF), D ** -0.5, 0.21875, ((1, 8),)),
        "up_bias": centred(splits[11], (LAYERS, FF), 1.0, 4.0, ((1, 8),)),
        "down_weight": centred(splits[12], (LAYERS, FF, D), FF ** -0.5, 0.109375, ((1, 8),)),
        "down_bias": centred(splits[13], (LAYERS, D), 1.0, 4.0, ((1, 8),)),
        "cotangent": centred(splits[14], (SEQS, LENGTH, D), 1.0, 6.0, ((0, 4), (1, 8))),
    }


epsilon = 1e-05
masked_value = -1e+30
maximum_precision = lax.Precision.HIGHEST

@jax.custom_vjp
def low(v):
    return lax.optimization_barrier(v.astype(jnp.bfloat16)).astype(jnp.float32)

@jax.custom_vjp
def low_back(v):
    return v

def low_keep(v):
    return (low(v), None)

def low_pass(kept, grad):
    return (grad,)

def back_keep(v):
    return (v, None)

def back_low(kept, grad):
    return (low(grad),)
low.defvjp(low_keep, low_pass)
low_back.defvjp(back_keep, back_low)

def norm_rows(values, gain, shift):
    centre = values - lax.optimization_barrier(jnp.mean(values, -1, keepdims=True))
    spread = lax.optimization_barrier(jnp.mean(centre * centre, -1, keepdims=True))
    return centre * lax.rsqrt(spread + epsilon) * gain + shift

def attend(parts):
    query, key_part, value_part = parts
    query_heads = query.reshape(LENGTH, HEADS, HEAD_DIM)
    key_heads = key_part.reshape(LENGTH, HEADS, HEAD_DIM)
    value_heads = value_part.reshape(LENGTH, HEADS, HEAD_DIM)
    scores = low_back(jnp.einsum('qhe,khe->hqk', query_heads, key_heads, precision=maximum_precision) * HEAD_DIM ** (-0.5))
    row_index = lax.broadcasted_iota(jnp.int32, (LENGTH, LENGTH), 0)
    col_index = lax.broadcasted_iota(jnp.int32, (LENGTH, LENGTH), 1)
    scores = jnp.where((row_index >= col_index)[None, :, :], scores, masked_value)
    probs = low(jax.nn.softmax(scores, axis=-1))
    attention_output = jnp.einsum('hqk,khe->qhe', probs, value_heads, precision=maximum_precision)
    return attention_output.reshape(LENGTH, D)

def one_block(current, params):
    gain_one, shift_one, query_key_value_weight, b_query, b_value, output_weight, output_proj_bias, gain_two, shift_two, up_weight, up_bias, down_weight, down_bias = params
    normalized_input = low(norm_rows(current, gain_one, shift_one))
    mixture_output = jnp.einsum('rbu,ua->rba', normalized_input, query_key_value_weight, precision=maximum_precision)
    query = low(low_back(mixture_output[..., :D] + b_query))
    key_part = low(low_back(mixture_output[..., D:2 * D]))
    value_part = low(low_back(mixture_output[..., 2 * D:] + b_value))
    attention_output = lax.map(jax.checkpoint(attend), (query, key_part, value_part))
    attention_output = low(low_back(attention_output))
    residual_branch = low_back(jnp.einsum('rbu,ua->rba', attention_output, output_weight, precision=maximum_precision) + output_proj_bias)
    x_mid = current + residual_branch
    shifted_values = low(norm_rows(x_mid, gain_two, shift_two))
    preactivation_values = low_back(jnp.einsum('vjo,op->vjp', shifted_values, up_weight, precision=maximum_precision) + up_bias)
    activation_values = low(jax.nn.gelu(preactivation_values, approximate=True))
    feedforward_output = low_back(jnp.einsum('zxm,mv->zxv', activation_values, down_weight, precision=maximum_precision) + down_bias)
    return x_mid + feedforward_output

def forward(current, *params):
    for depth_index in range(LAYERS):
        current = one_block(current, tuple((array[depth_index] for array in params)))
    return current

def reference(tokens, gain_one, shift_one, query_key_value_weight, b_query, b_value, output_weight, output_proj_bias, gain_two, shift_two, up_weight, up_bias, down_weight, down_bias, cotangent):
    params = tuple((array.astype(jnp.float32) for array in (gain_one, shift_one, query_key_value_weight, b_query, b_value, output_weight, output_proj_bias, gain_two, shift_two, up_weight, up_bias, down_weight, down_bias)))
    result, pullback = jax.vjp(forward, tokens.astype(jnp.float32), *params)
    grads = pullback(cotangent.astype(jnp.float32))
    return (result.astype(jnp.bfloat16), grads[0], grads[1], grads[2], grads[3], grads[4], grads[5], grads[6], grads[7], grads[8], grads[9], grads[10], grads[11], grads[12], grads[13])
```

```python
import functools

import jax
import jax.numpy as jnp
from jax import lax
from jax.experimental import pallas as pl
from jax.experimental.pallas import tpu as pltpu
from jax.sharding import PartitionSpec as P

HEADS = 12
HEAD_DIM = 64
EPSILON = 1e-05
MASKED = -1e30
F32 = jnp.float32
BF16 = jnp.bfloat16
BOTH = ("replica", "shard")
QUERY_ROWS = 256


def dot(a, b, contract):
    return lax.dot_general(a, b, (contract, ((), ())), preferred_element_type=F32)


def norm_rows(values, gain, shift):
    centre = values - jnp.mean(values, -1, keepdims=True)
    spread = jnp.mean(centre * centre, -1, keepdims=True)
    return centre * lax.rsqrt(spread + EPSILON) * gain + shift


def block_probs(q_ref, k_ref, head, first, rows):
    count = first + rows
    query = q_ref[head, first:count, :]
    keys = k_ref[head, 0:count, :]
    scores = dot(query, keys, ((1,), (1,))) * (HEAD_DIM**-0.5)
    row = lax.broadcasted_iota(jnp.int32, (rows, count), 0) + first
    col = lax.broadcasted_iota(jnp.int32, (rows, count), 1)
    scores = jnp.where(row >= col, scores, MASKED)
    expo = jnp.exp(scores - jnp.max(scores, -1, keepdims=True))
    return expo / jnp.sum(expo, -1, keepdims=True), query, keys


def split_heads(source, places):
    for place, target in enumerate(places):
        heads = target.shape[0]
        for head in range(heads):
            start = (place * heads + head) * HEAD_DIM
            target[head] = source[:, start : start + HEAD_DIM]


def attend_kernel(mixed_ref, out_ref, q_ref, k_ref, v_ref, o_ref):
    heads, length, _ = q_ref.shape
    rows = min(QUERY_ROWS, length)
    split_heads(mixed_ref, (q_ref, k_ref, v_ref))

    @pl.loop(0, heads)
    def _(head):
        for first in range(0, length, rows):
            probs, _, _ = block_probs(q_ref, k_ref, head, first, rows)
            o_ref[head, first : first + rows, :] = dot(
                probs.astype(BF16), v_ref[head, 0 : first + rows, :], ((1,), (0,))
            ).astype(BF16)

    for head in range(heads):
        out_ref[:, head * HEAD_DIM : (head + 1) * HEAD_DIM] = o_ref[head]


def attend(mixed, heads):
    length = mixed.shape[0]
    part = pltpu.VMEM((heads, length, HEAD_DIM), BF16)
    return pl.pallas_call(
        attend_kernel,
        out_shape=jax.ShapeDtypeStruct((length, heads * HEAD_DIM), BF16),
        in_specs=[pl.BlockSpec(memory_space=pltpu.VMEM)],
        out_specs=pl.BlockSpec(memory_space=pltpu.VMEM),
        scratch_shapes=[part, part, part, part],
        name="attend",
    )(mixed)


def attend_back_kernel(
    mixed_ref, d_ref, out_ref, q_ref, k_ref, v_ref, do_ref, dq_ref, dk_ref, dv_ref
):
    heads, length, _ = q_ref.shape
    rows = min(QUERY_ROWS, length)
    split_heads(mixed_ref, (q_ref, k_ref, v_ref))
    split_heads(d_ref, (do_ref,))

    @pl.loop(0, heads)
    def _(head):
        dk_ref[head] = jnp.zeros((length, HEAD_DIM), F32)
        dv_ref[head] = jnp.zeros((length, HEAD_DIM), F32)
        for first in range(0, length, rows):
            count = first + rows
            probs, query, keys = block_probs(q_ref, k_ref, head, first, rows)
            d_out = do_ref[head, first:count, :]
            d_probs = dot(d_out, v_ref[head, 0:count, :], ((1,), (1,)))
            row_dot = jnp.sum(d_probs * probs, -1, keepdims=True)
            d_scores = (probs * (d_probs - row_dot) * (HEAD_DIM**-0.5)).astype(BF16)
            dq_ref[head, first:count, :] = dot(d_scores, keys, ((1,), (0,))).astype(BF16)
            dk_ref[head, 0:count, :] += dot(d_scores, query, ((0,), (0,)))
            dv_ref[head, 0:count, :] += dot(probs.astype(BF16), d_out, ((0,), (0,)))

    for head in range(heads):
        for place, part in enumerate((dq_ref, dk_ref, dv_ref)):
            start = (place * heads + head) * HEAD_DIM
            out_ref[:, start : start + HEAD_DIM] = part[head].astype(BF16)


def attend_back(mixed, d_attended, heads):
    length = mixed.shape[0]
    part = pltpu.VMEM((heads, length, HEAD_DIM), BF16)
    wide = pltpu.VMEM((heads, length, HEAD_DIM), F32)
    return pl.pallas_call(
        attend_back_kernel,
        out_shape=jax.ShapeDtypeStruct((length, 3 * heads * HEAD_DIM), BF16),
        in_specs=[pl.BlockSpec(memory_space=pltpu.VMEM)] * 2,
        out_specs=pl.BlockSpec(memory_space=pltpu.VMEM),
        scratch_shapes=[part, part, part, part, part, wide, wide],
        name="attend_back",
    )(mixed, d_attended)


class Place:
    def __init__(self, tokens):
        self.replicas = lax.axis_size("replica")
        self.shards = lax.axis_size("shard")
        self.r = lax.axis_index("replica")
        self.s = lax.axis_index("shard")
        self.held, self.rows, self.width = tokens.shape
        self.heads = -(-HEADS // self.replicas)
        self.padded = self.heads * self.replicas
        assert self.held * self.replicas == self.shards

    def to_sequences(self, blocks):
        held = self.held
        got = []
        for turn in range(held):
            pairs = []
            for r in range(self.replicas):
                for s in range(self.shards):
                    pick = (s + turn) % held
                    target = (s // held) * self.shards + held * r + pick
                    pairs.append((r * self.shards + s, target))
            block = lax.dynamic_index_in_dim(blocks, (self.s + turn) % held, 0, keepdims=False)
            got.append(lax.ppermute(block, BOTH, pairs))
        stacked = jnp.stack(got)
        ordered = [
            lax.dynamic_index_in_dim(stacked, (self.s - u) % held, 0, keepdims=False)
            for u in range(held)
        ]
        return jnp.concatenate(ordered, 0)

    def from_sequences(self, values):
        held, rows = self.held, self.rows
        blocks = values.reshape(held, rows, values.shape[-1])
        got = []
        for turn in range(held):
            pairs = []
            for r in range(self.replicas):
                for s in range(self.shards):
                    pick = (s + turn) % held
                    target = (s // held) * self.shards + held * r + pick
                    pairs.append((target, r * self.shards + s))
            block = lax.dynamic_index_in_dim(blocks, (self.s - turn) % held, 0, keepdims=False)
            got.append(lax.ppermute(block, BOTH, pairs))
        stacked = jnp.stack(got)
        return jnp.stack(
            [
                lax.dynamic_index_in_dim(stacked, (i - self.s) % held, 0, keepdims=False)
                for i in range(held)
            ]
        )

    def to_heads(self, values):
        return lax.all_to_all(values, "replica", 1, 0, tiled=True)

    def to_rows(self, values):
        return lax.all_to_all(values, "replica", 0, 1, tiled=True)

    def mix_columns(self, weight):
        lead = weight.shape[:-1]
        parts = weight.reshape(lead + (3, HEADS, HEAD_DIM))
        extra = [(0, 0)] * len(lead) + [(0, 0), (0, self.padded - HEADS), (0, 0)]
        parts = jnp.pad(parts, extra)
        parts = parts.reshape(lead + (3, self.replicas, self.heads * HEAD_DIM))
        return jnp.swapaxes(parts, -3, -2).reshape(lead + (-1,))

    def unmix_columns(self, values):
        lead = values.shape[:-1]
        parts = values.reshape(lead + (self.replicas, 3, self.heads * HEAD_DIM))
        parts = jnp.swapaxes(parts, -3, -2).reshape(lead + (3, self.padded, HEAD_DIM))
        return parts[..., :HEADS, :].reshape(lead + (-1,))


def gather_vectors(place, vectors):
    layers = vectors[0].shape[0]
    packed = jnp.concatenate(vectors, -1)
    whole = lax.all_gather(packed, "shard", axis=0)
    out, start = [], 0
    for vector in vectors:
        size = vector.shape[1]
        piece = whole[:, :, start : start + size]
        out.append(jnp.swapaxes(piece, 0, 1).reshape(layers, -1).astype(F32))
        start += size
    return out


def gather_weights(place, mix, out_w, up, down):
    full = [
        [lax.all_gather(w[layer], "shard", axis=0, tiled=True) for w in (mix, out_w, up, down)]
        for layer in range(mix.shape[0])
    ]
    return full


def reduce_weights(place, grads):
    return [
        lax.psum(
            lax.psum_scatter(g, "shard", scatter_dimension=0, tiled=True).astype(F32), "replica"
        )
        for g in grads
    ]


def forward_block(place, current, weights, vectors):
    mix, out_w, up, down = weights
    gain_one, shift_one, mix_bias, out_bias, gain_two, shift_two, up_bias, down_bias = vectors
    normed = norm_rows(current, gain_one, shift_one).astype(BF16)
    mixed = (dot(normed, mix, ((1,), (0,))) + mix_bias).astype(BF16)
    mixed = place.to_heads(mixed)
    attended = place.to_rows(attend(mixed, place.heads))[:, : place.width]
    x_mid = current + (dot(attended, out_w, ((1,), (0,))) + out_bias)
    moved = norm_rows(x_mid, gain_two, shift_two).astype(BF16)
    pre = dot(moved, up, ((1,), (0,))) + up_bias
    act = jax.nn.gelu(pre, approximate=True).astype(BF16)
    result = x_mid + dot(act, down, ((1,), (0,))) + down_bias
    return result, (current, normed, mixed, attended, x_mid, moved, pre, act)


def backward_block(place, grad_next, weights, vectors, saved):
    mix, out_w, up, down = weights
    gain_one, shift_one, mix_bias, out_bias, gain_two, shift_two, up_bias, down_bias = vectors
    current, normed, mixed, attended, x_mid, moved, pre, act = saved
    d_ffn = grad_next.astype(BF16)
    grad_down = dot(act, d_ffn, ((0,), (0,))).astype(BF16)
    grad_b_down = jnp.sum(d_ffn.astype(F32), 0)
    d_act = dot(d_ffn, down, ((1,), (1,)))
    gelu_back = jax.vjp(lambda inner: jax.nn.gelu(inner, approximate=True), pre)[1]
    d_pre = gelu_back(d_act)[0].astype(BF16)
    grad_up = dot(moved, d_pre, ((0,), (0,))).astype(BF16)
    grad_b_up = jnp.sum(d_pre.astype(F32), 0)
    d_moved = dot(d_pre, up, ((1,), (1,)))
    norm_back = jax.vjp(norm_rows, x_mid, gain_two, shift_two)[1]
    d_from_norm, grad_gain_two, grad_shift_two = norm_back(d_moved)
    grad_mid = grad_next + d_from_norm
    d_branch = grad_mid.astype(BF16)
    grad_out = dot(attended, d_branch, ((0,), (0,))).astype(BF16)
    grad_b_out = jnp.sum(d_branch.astype(F32), 0)
    d_att = dot(d_branch, out_w, ((1,), (1,))).astype(BF16)
    d_att = jnp.pad(d_att, ((0, 0), (0, place.padded * HEAD_DIM - place.width)))
    d_mixed = place.to_rows(attend_back(mixed, place.to_heads(d_att), place.heads))
    grad_mix = dot(normed, d_mixed, ((0,), (0,))).astype(BF16)
    grad_b_mix = place.unmix_columns(jnp.sum(d_mixed.astype(F32), 0))
    grad_b_query = grad_b_mix[: place.width]
    grad_b_value = grad_b_mix[2 * place.width :]
    d_normed = dot(d_mixed, mix, ((1,), (1,)))
    first_back = jax.vjp(norm_rows, current, gain_one, shift_one)[1]
    d_from_first, grad_gain_one, grad_shift_one = first_back(d_normed)
    grad_current = grad_mid + d_from_first
    grad_vectors = (
        grad_gain_one,
        grad_shift_one,
        grad_b_query,
        grad_b_value,
        grad_b_out,
        grad_gain_two,
        grad_shift_two,
        grad_b_up,
        grad_b_down,
    )
    return grad_current, (grad_mix, grad_out, grad_up, grad_down), grad_vectors


def per_device(
    tokens,
    gain_one,
    shift_one,
    query_key_value_weight,
    b_query,
    b_value,
    output_weight,
    output_proj_bias,
    gain_two,
    shift_two,
    up_weight,
    up_bias,
    down_weight,
    down_bias,
    cotangent,
):
    place = Place(tokens)
    layers = gain_one.shape[0]
    mix_weight = place.mix_columns(query_key_value_weight)
    vectors = gather_vectors(
        place,
        (
            gain_one,
            shift_one,
            b_query,
            b_value,
            output_proj_bias,
            gain_two,
            shift_two,
            up_bias,
            down_bias,
        ),
    )
    g1, s1, bq, bv, bo, g2, s2, bu, bd = vectors
    mix_bias = place.mix_columns(jnp.concatenate([bq, jnp.zeros_like(bq), bv], -1))
    weights = gather_weights(place, mix_weight, output_weight, up_weight, down_weight)

    def layer_vectors(n):
        return (g1[n], s1[n], mix_bias[n], bo[n], g2[n], s2[n], bu[n], bd[n])

    current = place.to_sequences(tokens).astype(F32)
    saved = []
    for n in range(layers):
        current, kept = forward_block(place, current, weights[n], layer_vectors(n))
        saved.append(kept)
    output = place.from_sequences(current.astype(BF16))
    grad_now = place.to_sequences(cotangent).astype(F32)
    weight_grads, vector_grads = [None] * layers, [None] * layers
    for n in reversed(range(layers)):
        grad_now, local, vector_grads[n] = backward_block(
            place, grad_now, weights[n], layer_vectors(n), saved[n]
        )
        weight_grads[n] = reduce_weights(place, local)
    grad_tokens = place.from_sequences(grad_now.astype(BF16)).astype(F32)
    grad_mix, grad_out, grad_up, grad_down = (
        jnp.stack([weight_grads[n][m] for n in range(layers)]) for m in range(4)
    )
    grad_mix = place.unmix_columns(grad_mix)
    sizes = [v.shape[0] for v in vector_grads[0]]
    packed = jnp.stack([jnp.concatenate(v) for v in vector_grads])
    packed = lax.psum(packed, BOTH)
    own, start = [], 0
    for size in sizes:
        part = size // place.shards
        own.append(lax.dynamic_slice_in_dim(packed, start + place.s * part, part, 1))
        start += size
    (
        grad_gain_one,
        grad_shift_one,
        grad_b_query,
        grad_b_value,
        grad_b_out,
        grad_gain_two,
        grad_shift_two,
        grad_b_up,
        grad_b_down,
    ) = own
    return (
        output,
        grad_tokens,
        grad_gain_one,
        grad_shift_one,
        grad_mix,
        grad_b_query,
        grad_b_value,
        grad_out,
        grad_b_out,
        grad_gain_two,
        grad_shift_two,
        grad_up,
        grad_b_up,
        grad_down,
        grad_b_down,
    )


def solution(mesh):
    vector, matrix = P(None, "shard"), P(None, "shard", None)
    rows = P("replica", "shard", None)
    in_specs = (
        rows,
        vector,
        vector,
        matrix,
        vector,
        vector,
        matrix,
        vector,
        vector,
        vector,
        matrix,
        vector,
        matrix,
        vector,
        rows,
    )
    out_specs = (
        rows,
        rows,
        vector,
        vector,
        matrix,
        vector,
        vector,
        matrix,
        vector,
        vector,
        vector,
        matrix,
        vector,
        matrix,
        vector,
    )
    return jax.shard_map(
        per_device, mesh=mesh, in_specs=in_specs, out_specs=out_specs, check_vma=False
    )
```

```python
import functools

import jax
import jax.numpy as jnp
from jax import lax
from jax.experimental import pallas as pl
from jax.experimental.pallas import tpu as pltpu
from jax.sharding import PartitionSpec as P

HEADS = 12
HEAD_DIM = 64
EPSILON = 1e-05
MASKED = -1e30
F32 = jnp.float32
BF16 = jnp.bfloat16
BOTH = ("replica", "shard")
QUERY_ROWS = 256


def dot(a, b, contract):
    return lax.dot_general(a, b, (contract, ((), ())), preferred_element_type=F32)


def norm_rows(values, gain, shift):
    centre = values - jnp.mean(values, -1, keepdims=True)
    spread = jnp.mean(centre * centre, -1, keepdims=True)
    return centre * lax.rsqrt(spread + EPSILON) * gain + shift


def block_probs(q_ref, k_ref, head, first, rows):
    count = first + rows
    query = q_ref[head, first:count, :]
    keys = k_ref[head, 0:count, :]
    scores = dot(query, keys, ((1,), (1,))) * (HEAD_DIM**-0.5)
    row = lax.broadcasted_iota(jnp.int32, (rows, count), 0) + first
    col = lax.broadcasted_iota(jnp.int32, (rows, count), 1)
    scores = jnp.where(row >= col, scores, MASKED)
    expo = jnp.exp(scores - jnp.max(scores, -1, keepdims=True))
    return expo / jnp.sum(expo, -1, keepdims=True), query, keys


def split_heads(source, places):
    for place, target in enumerate(places):
        heads = target.shape[0]
        for head in range(heads):
            start = (place * heads + head) * HEAD_DIM
            target[head] = source[:, start : start + HEAD_DIM]


def attend_kernel(mixed_ref, out_ref, q_ref, k_ref, v_ref, o_ref):
    heads, length, _ = q_ref.shape
    rows = min(QUERY_ROWS, length)
    split_heads(mixed_ref, (q_ref, k_ref, v_ref))

    @pl.loop(0, heads)
    def _(head):
        for first in range(0, length, rows):
            probs, _, _ = block_probs(q_ref, k_ref, head, first, rows)
            o_ref[head, first : first + rows, :] = dot(
                probs.astype(BF16), v_ref[head, 0 : first + rows, :], ((1,), (0,))
            ).astype(BF16)

    for head in range(heads):
        out_ref[:, head * HEAD_DIM : (head + 1) * HEAD_DIM] = o_ref[head]


def attend(mixed, heads):
    length = mixed.shape[0]
    part = pltpu.VMEM((heads, length, HEAD_DIM), BF16)
    return pl.pallas_call(
        attend_kernel,
        out_shape=jax.ShapeDtypeStruct((length, heads * HEAD_DIM), BF16),
        in_specs=[pl.BlockSpec(memory_space=pltpu.VMEM)],
        out_specs=pl.BlockSpec(memory_space=pltpu.VMEM),
        scratch_shapes=[part, part, part, part],
        name="attend",
    )(mixed)


def attend_back_kernel(
    mixed_ref, d_ref, out_ref, q_ref, k_ref, v_ref, do_ref, dq_ref, dk_ref, dv_ref
):
    heads, length, _ = q_ref.shape
    rows = min(QUERY_ROWS, length)
    split_heads(mixed_ref, (q_ref, k_ref, v_ref))
    split_heads(d_ref, (do_ref,))

    @pl.loop(0, heads)
    def _(head):
        dk_ref[head] = jnp.zeros((length, HEAD_DIM), F32)
        dv_ref[head] = jnp.zeros((length, HEAD_DIM), F32)
        for first in range(0, length, rows):
            count = first + rows
            probs, query, keys = block_probs(q_ref, k_ref, head, first, rows)
            d_out = do_ref[head, first:count, :]
            d_probs = dot(d_out, v_ref[head, 0:count, :], ((1,), (1,)))
            row_dot = jnp.sum(d_probs * probs, -1, keepdims=True)
            d_scores = (probs * (d_probs - row_dot) * (HEAD_DIM**-0.5)).astype(BF16)
            dq_ref[head, first:count, :] = dot(d_scores, keys, ((1,), (0,))).astype(BF16)
            dk_ref[head, 0:count, :] += dot(d_scores, query, ((0,), (0,)))
            dv_ref[head, 0:count, :] += dot(probs.astype(BF16), d_out, ((0,), (0,)))

    for head in range(heads):
        for place, part in enumerate((dq_ref, dk_ref, dv_ref)):
            start = (place * heads + head) * HEAD_DIM
            out_ref[:, start : start + HEAD_DIM] = part[head].astype(BF16)


def attend_back(mixed, d_attended, heads):
    length = mixed.shape[0]
    part = pltpu.VMEM((heads, length, HEAD_DIM), BF16)
    wide = pltpu.VMEM((heads, length, HEAD_DIM), F32)
    return pl.pallas_call(
        attend_back_kernel,
        out_shape=jax.ShapeDtypeStruct((length, 3 * heads * HEAD_DIM), BF16),
        in_specs=[pl.BlockSpec(memory_space=pltpu.VMEM)] * 2,
        out_specs=pl.BlockSpec(memory_space=pltpu.VMEM),
        scratch_shapes=[part, part, part, part, part, wide, wide],
        name="attend_back",
    )(mixed, d_attended)


class Place:
    def __init__(self, tokens):
        self.replicas = lax.axis_size("replica")
        self.shards = lax.axis_size("shard")
        self.r = lax.axis_index("replica")
        self.s = lax.axis_index("shard")
        self.held, self.rows, self.width = tokens.shape
        self.heads = -(-HEADS // self.replicas)
        self.padded = self.heads * self.replicas
        assert self.held * self.replicas == self.shards

    def to_sequences(self, blocks):
        held = self.held
        got = []
        for turn in range(held):
            pairs = []
            for r in range(self.replicas):
                for s in range(self.shards):
                    pick = (s + turn) % held
                    target = (s // held) * self.shards + held * r + pick
                    pairs.append((r * self.shards + s, target))
            block = lax.dynamic_index_in_dim(blocks, (self.s + turn) % held, 0, keepdims=False)
            got.append(lax.ppermute(block, BOTH, pairs))
        stacked = jnp.stack(got)
        ordered = [
            lax.dynamic_index_in_dim(stacked, (self.s - u) % held, 0, keepdims=False)
            for u in range(held)
        ]
        return jnp.concatenate(ordered, 0)

    def from_sequences(self, values):
        held, rows = self.held, self.rows
        blocks = values.reshape(held, rows, values.shape[-1])
        got = []
        for turn in range(held):
            pairs = []
            for r in range(self.replicas):
                for s in range(self.shards):
                    pick = (s + turn) % held
                    target = (s // held) * self.shards + held * r + pick
                    pairs.append((target, r * self.shards + s))
            block = lax.dynamic_index_in_dim(blocks, (self.s - turn) % held, 0, keepdims=False)
            got.append(lax.ppermute(block, BOTH, pairs))
        stacked = jnp.stack(got)
        return jnp.stack(
            [
                lax.dynamic_index_in_dim(stacked, (i - self.s) % held, 0, keepdims=False)
                for i in range(held)
            ]
        )

    def to_heads(self, values):
        return lax.all_to_all(values, "replica", 1, 0, tiled=True)

    def to_rows(self, values):
        return lax.all_to_all(values, "replica", 0, 1, tiled=True)

    def mix_columns(self, weight):
        lead = weight.shape[:-1]
        parts = weight.reshape(lead + (3, HEADS, HEAD_DIM))
        extra = [(0, 0)] * len(lead) + [(0, 0), (0, self.padded - HEADS), (0, 0)]
        parts = jnp.pad(parts, extra)
        parts = parts.reshape(lead + (3, self.replicas, self.heads * HEAD_DIM))
        return jnp.swapaxes(parts, -3, -2).reshape(lead + (-1,))

    def unmix_columns(self, values):
        lead = values.shape[:-1]
        parts = values.reshape(lead + (self.replicas, 3, self.heads * HEAD_DIM))
        parts = jnp.swapaxes(parts, -3, -2).reshape(lead + (3, self.padded, HEAD_DIM))
        return parts[..., :HEADS, :].reshape(lead + (-1,))


MESH = pl.DeviceIdType.MESH


class Grid:
    def __init__(self, replicas, shards):
        self.cores = 2 if replicas % 2 == 0 else 1
        self.xs = replicas // self.cores
        self.zs = 4 if shards % 4 == 0 else 1
        self.ys = shards // self.zs
        r, s = lax.axis_index("replica"), lax.axis_index("shard")
        self.x, self.core = r // self.cores, lax.rem(r, self.cores)
        self.z, self.y = s // self.ys, lax.rem(s, self.ys)

    def device(self, x=0, core=0, z=0, y=0):
        to_x = lax.rem(self.x + x + self.xs, self.xs)
        to_core = lax.rem(self.core + core, self.cores)
        to_z = lax.rem(self.z + z + self.zs, self.zs)
        to_y = lax.rem(self.y + y + self.ys, self.ys)
        return {"replica": to_x * self.cores + to_core, "shard": to_z * self.ys + to_y}

    def block(self, z_back, y_back):
        from_z = lax.rem(self.z - z_back + self.zs, self.zs)
        from_y = lax.rem(self.y - y_back + self.ys, self.ys)
        return from_z * self.ys + from_y

    def greet(self):
        near = []
        for axis, size in (("x", self.xs), ("core", self.cores), ("z", self.zs), ("y", self.ys)):
            if size > 1:
                near.append({axis: 1})
            if size > 2:
                near.append({axis: -1})
        barrier = pltpu.get_barrier_semaphore()
        for step in near:
            pl.semaphore_signal(barrier, 1, device_id=self.device(**step), device_id_type=MESH)
        pl.semaphore_wait(barrier, len(near))


def window(ref, row, rows, col, cols):
    row = row if isinstance(row, int) else pl.multiple_of(row, 16)
    col = col if isinstance(col, int) else pl.multiple_of(col, 128)
    return ref.at[pl.ds(row, rows), pl.ds(col, cols)]


def part_of(grid, kind, ref, shape, block, x_at):
    rows, cols = shape
    row = block * rows
    if kind == "whole":
        return window(ref, row, rows, 0, cols)
    half = cols // grid.cores
    if kind == "half":
        return window(ref, row, rows, grid.core * half, half)
    if kind == "columns":
        share = half // grid.xs
        return window(ref, row, rows, grid.core * half + x_at * share, share)
    share = rows // grid.xs
    return window(ref, row + x_at * share, share, grid.core * half, half)


def half_of(grid, ref, shape, block):
    rows, cols = shape
    half = cols // grid.cores
    return window(ref, block * rows, rows, grid.core * half, half)


def copies_of_gather(kind, grid):
    blocks = grid.zs * grid.ys
    count = blocks - 1
    if kind in ("columns", "rows"):
        count += (blocks - 1) * (grid.xs - 1)
    if kind != "whole":
        count += (blocks - 1) * (grid.cores - 1)
    return count


def gather_kernel(replicas, shards, kinds, *refs):
    count = len(kinds)
    sources, targets = refs[:count], refs[count : 2 * count]
    send_sems, recv_sems, own_sems = refs[2 * count :]
    grid = Grid(replicas, shards)
    shapes = [source.shape for source in sources]
    started = []

    def send(source, target, device):
        at = len(started)
        copy = pltpu.make_async_remote_copy(
            src_ref=source,
            dst_ref=target,
            send_sem=send_sems.at[at],
            recv_sem=recv_sems.at[at],
            device_id=device,
            device_id_type=MESH,
        )
        copy.start()
        started.append(copy)
        return copy

    def fetched(job, z_back, y_back, x_back=0):
        kind, shape = kinds[job], shapes[job]
        x_at = lax.rem(grid.x - x_back + grid.xs, grid.xs)
        target = part_of(grid, kind, targets[job], shape, grid.block(z_back, y_back), x_at)
        if z_back == 0 and y_back == 0:
            return part_of(grid, kind, sources[job], shape, 0, x_at), target
        return target, target

    grid.greet()
    own = []
    for job in range(count):
        rows = shapes[job][0]
        place = targets[job].at[pl.ds(pl.multiple_of(grid.block(0, 0) * rows, 16), rows), :]
        copy = pltpu.make_async_copy(sources[job], place, own_sems.at[job])
        copy.start()
        own.append(copy)

    along_z, along_y, along_x, along_core = {}, {}, {}, {}
    for step in range(grid.zs + 3):
        for job, kind in enumerate(kinds):
            z_back = step
            if z_back < grid.zs:
                if z_back > 0:
                    along_z[job, z_back - 1].wait_recv()
                if z_back < grid.zs - 1:
                    along_z[job, z_back] = send(*fetched(job, z_back, 0), grid.device(z=1))
                if grid.ys > 1:
                    along_y[job, z_back, 0] = send(*fetched(job, z_back, 0), grid.device(y=1))
            z_back = step - 1
            if 0 <= z_back < grid.zs:
                for y_back in range(1, grid.ys):
                    along_y[job, z_back, y_back - 1].wait_recv()
                    if y_back < grid.ys - 1:
                        along_y[job, z_back, y_back] = send(
                            *fetched(job, z_back, y_back), grid.device(y=1)
                        )
                if kind in ("columns", "rows") and grid.xs > 1:
                    for y_back in range(0 if z_back else 1, grid.ys):
                        along_x[job, z_back, y_back, 0] = send(
                            *fetched(job, z_back, y_back), grid.device(x=1)
                        )
            z_back = step - 2
            if 0 <= z_back < grid.zs and kind != "whole":
                for y_back in range(0 if z_back else 1, grid.ys):
                    if kind != "half":
                        for x_back in range(1, grid.xs):
                            along_x[job, z_back, y_back, x_back - 1].wait_recv()
                            if x_back < grid.xs - 1:
                                along_x[job, z_back, y_back, x_back] = send(
                                    *fetched(job, z_back, y_back, x_back), grid.device(x=1)
                                )
                    if grid.cores > 1:
                        half = half_of(grid, targets[job], shapes[job], grid.block(z_back, y_back))
                        along_core[job, z_back, y_back] = send(half, half, grid.device(core=1))
            z_back = step - 3
            if 0 <= z_back < grid.zs and kind != "whole" and grid.cores > 1:
                for y_back in range(0 if z_back else 1, grid.ys):
                    along_core[job, z_back, y_back].wait_recv()
    for copy in started:
        copy.wait_send()
    for copy in own:
        copy.wait()


def gather_shards(place, kinds, shards):
    sizes = Grid(place.replicas, place.shards)
    copies = sum(copies_of_gather(kind, sizes) for kind in kinds)
    return pl.pallas_call(
        functools.partial(gather_kernel, place.replicas, place.shards, kinds),
        out_shape=[
            jax.ShapeDtypeStruct((place.shards * a.shape[0], a.shape[1]), a.dtype) for a in shards
        ],
        in_specs=[pl.BlockSpec(memory_space=pltpu.VMEM)] * len(shards),
        out_specs=[pl.BlockSpec(memory_space=pl.ANY)] * len(shards),
        scratch_shapes=[
            pltpu.SemaphoreType.DMA((copies,)),
            pltpu.SemaphoreType.DMA((copies,)),
            pltpu.SemaphoreType.DMA((len(shards),)),
        ],
        compiler_params=pltpu.CompilerParams(collective_id=0, has_side_effects=True),
        name="gather_shards",
    )(*shards)


def gather_all(place, vectors, mix, out_w, up, down):
    layers = mix.shape[0]
    packed = jnp.concatenate(vectors, -1).reshape(-1)
    size = packed.shape[0]
    lanes = 128 * -(-size // (16 * 128))
    packed = jnp.pad(packed, (0, 16 * lanes - size)).reshape(16, lanes)
    first = jnp.concatenate([mix, out_w], -1)
    kinds, shards = ["whole"], [packed]
    for layer in range(layers):
        kinds += ["half", "columns", "rows"]
        shards += [first[layer], up[layer], down[layer]]
    whole = gather_shards(place, tuple(kinds), shards)
    flat = whole[0].reshape(place.shards, -1)[:, :size].reshape(place.shards, layers, -1)
    out, start = [], 0
    for vector in vectors:
        piece = flat[:, :, start : start + vector.shape[1]]
        out.append(jnp.swapaxes(piece, 0, 1).reshape(layers, -1).astype(F32))
        start += vector.shape[1]
    return [whole[1 + 3 * n : 4 + 3 * n] for n in range(layers)], out


def reduce_weights(place, grads):
    return [
        lax.psum(
            lax.psum_scatter(g, "shard", scatter_dimension=0, tiled=True).astype(F32), "replica"
        )
        for g in grads
    ]


def forward_block(place, current, weights, vectors):
    mix_out, up, down = weights
    mix, out_w = jnp.split(mix_out, [mix_out.shape[1] - place.width], 1)
    gain_one, shift_one, mix_bias, out_bias, gain_two, shift_two, up_bias, down_bias = vectors
    normed = norm_rows(current, gain_one, shift_one).astype(BF16)
    mixed = (dot(normed, mix, ((1,), (0,))) + mix_bias).astype(BF16)
    mixed = place.to_heads(mixed)
    attended = place.to_rows(attend(mixed, place.heads))[:, : place.width]
    x_mid = current + (dot(attended, out_w, ((1,), (0,))) + out_bias)
    moved = norm_rows(x_mid, gain_two, shift_two).astype(BF16)
    pre = dot(moved, up, ((1,), (0,))) + up_bias
    act = jax.nn.gelu(pre, approximate=True).astype(BF16)
    result = x_mid + dot(act, down, ((1,), (0,))) + down_bias
    return result, (current, normed, mixed, attended, x_mid, moved, pre, act)


def backward_block(place, grad_next, weights, vectors, saved):
    mix_out, up, down = weights
    mix, out_w = jnp.split(mix_out, [mix_out.shape[1] - place.width], 1)
    gain_one, shift_one, mix_bias, out_bias, gain_two, shift_two, up_bias, down_bias = vectors
    current, normed, mixed, attended, x_mid, moved, pre, act = saved
    d_ffn = grad_next.astype(BF16)
    grad_down = dot(act, d_ffn, ((0,), (0,))).astype(BF16)
    grad_b_down = jnp.sum(d_ffn.astype(F32), 0)
    d_act = dot(d_ffn, down, ((1,), (1,)))
    gelu_back = jax.vjp(lambda inner: jax.nn.gelu(inner, approximate=True), pre)[1]
    d_pre = gelu_back(d_act)[0].astype(BF16)
    grad_up = dot(moved, d_pre, ((0,), (0,))).astype(BF16)
    grad_b_up = jnp.sum(d_pre.astype(F32), 0)
    d_moved = dot(d_pre, up, ((1,), (1,)))
    norm_back = jax.vjp(norm_rows, x_mid, gain_two, shift_two)[1]
    d_from_norm, grad_gain_two, grad_shift_two = norm_back(d_moved)
    grad_mid = grad_next + d_from_norm
    d_branch = grad_mid.astype(BF16)
    grad_out = dot(attended, d_branch, ((0,), (0,))).astype(BF16)
    grad_b_out = jnp.sum(d_branch.astype(F32), 0)
    d_att = dot(d_branch, out_w, ((1,), (1,))).astype(BF16)
    d_att = jnp.pad(d_att, ((0, 0), (0, place.padded * HEAD_DIM - place.width)))
    d_mixed = place.to_rows(attend_back(mixed, place.to_heads(d_att), place.heads))
    grad_mix = dot(normed, d_mixed, ((0,), (0,))).astype(BF16)
    grad_b_mix = place.unmix_columns(jnp.sum(d_mixed.astype(F32), 0))
    grad_b_query = grad_b_mix[: place.width]
    grad_b_value = grad_b_mix[2 * place.width :]
    d_normed = dot(d_mixed, mix, ((1,), (1,)))
    first_back = jax.vjp(norm_rows, current, gain_one, shift_one)[1]
    d_from_first, grad_gain_one, grad_shift_one = first_back(d_normed)
    grad_current = grad_mid + d_from_first
    grad_vectors = (
        grad_gain_one,
        grad_shift_one,
        grad_b_query,
        grad_b_value,
        grad_b_out,
        grad_gain_two,
        grad_shift_two,
        grad_b_up,
        grad_b_down,
    )
    return grad_current, (grad_mix, grad_out, grad_up, grad_down), grad_vectors


def per_device(
    tokens,
    gain_one,
    shift_one,
    query_key_value_weight,
    b_query,
    b_value,
    output_weight,
    output_proj_bias,
    gain_two,
    shift_two,
    up_weight,
    up_bias,
    down_weight,
    down_bias,
    cotangent,
):
    place = Place(tokens)
    layers = gain_one.shape[0]
    mix_weight = place.mix_columns(query_key_value_weight)
    weights, vectors = gather_all(
        place,
        (
            gain_one,
            shift_one,
            b_query,
            b_value,
            output_proj_bias,
            gain_two,
            shift_two,
            up_bias,
            down_bias,
        ),
        mix_weight,
        output_weight,
        up_weight,
        down_weight,
    )
    g1, s1, bq, bv, bo, g2, s2, bu, bd = vectors
    mix_bias = place.mix_columns(jnp.concatenate([bq, jnp.zeros_like(bq), bv], -1))

    def layer_vectors(n):
        return (g1[n], s1[n], mix_bias[n], bo[n], g2[n], s2[n], bu[n], bd[n])

    current = place.to_sequences(tokens).astype(F32)
    saved = []
    for n in range(layers):
        current, kept = forward_block(place, current, weights[n], layer_vectors(n))
        saved.append(kept)
    output = place.from_sequences(current.astype(BF16))
    grad_now = place.to_sequences(cotangent).astype(F32)
    weight_grads, vector_grads = [None] * layers, [None] * layers
    for n in reversed(range(layers)):
        grad_now, local, vector_grads[n] = backward_block(
            place, grad_now, weights[n], layer_vectors(n), saved[n]
        )
        weight_grads[n] = reduce_weights(place, local)
    grad_tokens = place.from_sequences(grad_now.astype(BF16)).astype(F32)
    grad_mix, grad_out, grad_up, grad_down = (
        jnp.stack([weight_grads[n][m] for n in range(layers)]) for m in range(4)
    )
    grad_mix = place.unmix_columns(grad_mix)
    sizes = [v.shape[0] for v in vector_grads[0]]
    packed = jnp.stack([jnp.concatenate(v) for v in vector_grads])
    packed = lax.psum(packed, BOTH)
    own, start = [], 0
    for size in sizes:
        part = size // place.shards
        own.append(lax.dynamic_slice_in_dim(packed, start + place.s * part, part, 1))
        start += size
    (
        grad_gain_one,
        grad_shift_one,
        grad_b_query,
        grad_b_value,
        grad_b_out,
        grad_gain_two,
        grad_shift_two,
        grad_b_up,
        grad_b_down,
    ) = own
    return (
        output,
        grad_tokens,
        grad_gain_one,
        grad_shift_one,
        grad_mix,
        grad_b_query,
        grad_b_value,
        grad_out,
        grad_b_out,
        grad_gain_two,
        grad_shift_two,
        grad_up,
        grad_b_up,
        grad_down,
        grad_b_down,
    )


def solution(mesh):
    vector, matrix = P(None, "shard"), P(None, "shard", None)
    rows = P("replica", "shard", None)
    in_specs = (
        rows,
        vector,
        vector,
        matrix,
        vector,
        vector,
        matrix,
        vector,
        vector,
        vector,
        matrix,
        vector,
        matrix,
        vector,
        rows,
    )
    out_specs = (
        rows,
        rows,
        vector,
        vector,
        matrix,
        vector,
        vector,
        matrix,
        vector,
        vector,
        vector,
        matrix,
        vector,
        matrix,
        vector,
    )
    return jax.shard_map(
        per_device, mesh=mesh, in_specs=in_specs, out_specs=out_specs, check_vma=False
    )
```

```python
import functools

import jax
import jax.numpy as jnp
from jax import lax
from jax.experimental import pallas as pl
from jax.experimental.pallas import tpu as pltpu
from jax.sharding import PartitionSpec as P

HEADS = 12
HEAD_DIM = 64
EPSILON = 1e-05
MASKED = -1e30
F32 = jnp.float32
BF16 = jnp.bfloat16
BOTH = ("replica", "shard")
QUERY_ROWS = 256


def dot(a, b, contract):
    return lax.dot_general(a, b, (contract, ((), ())), preferred_element_type=F32)


def norm_rows(values, gain, shift):
    centre = values - jnp.mean(values, -1, keepdims=True)
    spread = jnp.mean(centre * centre, -1, keepdims=True)
    return centre * lax.rsqrt(spread + EPSILON) * gain + shift


def block_probs(q_ref, k_ref, head, first, rows):
    count = first + rows
    query = q_ref[head, first:count, :]
    keys = k_ref[head, 0:count, :]
    scores = dot(query, keys, ((1,), (1,))) * (HEAD_DIM**-0.5)
    row = lax.broadcasted_iota(jnp.int32, (rows, count), 0) + first
    col = lax.broadcasted_iota(jnp.int32, (rows, count), 1)
    scores = jnp.where(row >= col, scores, MASKED)
    expo = jnp.exp(scores - jnp.max(scores, -1, keepdims=True))
    return expo / jnp.sum(expo, -1, keepdims=True), query, keys


def split_heads(source, places):
    for place, target in enumerate(places):
        heads = target.shape[0]
        for head in range(heads):
            start = (place * heads + head) * HEAD_DIM
            target[head] = source[:, start : start + HEAD_DIM]


def attend_kernel(mixed_ref, out_ref, q_ref, k_ref, v_ref, o_ref):
    heads, length, _ = q_ref.shape
    rows = min(QUERY_ROWS, length)
    split_heads(mixed_ref, (q_ref, k_ref, v_ref))

    @pl.loop(0, heads)
    def _(head):
        for first in range(0, length, rows):
            probs, _, _ = block_probs(q_ref, k_ref, head, first, rows)
            o_ref[head, first : first + rows, :] = dot(
                probs.astype(BF16), v_ref[head, 0 : first + rows, :], ((1,), (0,))
            ).astype(BF16)

    for head in range(heads):
        out_ref[:, head * HEAD_DIM : (head + 1) * HEAD_DIM] = o_ref[head]


def attend(mixed, heads):
    length = mixed.shape[0]
    part = pltpu.VMEM((heads, length, HEAD_DIM), BF16)
    return pl.pallas_call(
        attend_kernel,
        out_shape=jax.ShapeDtypeStruct((length, heads * HEAD_DIM), BF16),
        in_specs=[pl.BlockSpec(memory_space=pltpu.VMEM)],
        out_specs=pl.BlockSpec(memory_space=pltpu.VMEM),
        scratch_shapes=[part, part, part, part],
        name="attend",
    )(mixed)


def attend_back_kernel(
    mixed_ref, d_ref, out_ref, q_ref, k_ref, v_ref, do_ref, dq_ref, dk_ref, dv_ref
):
    heads, length, _ = q_ref.shape
    rows = min(QUERY_ROWS, length)
    split_heads(mixed_ref, (q_ref, k_ref, v_ref))
    split_heads(d_ref, (do_ref,))

    @pl.loop(0, heads)
    def _(head):
        dk_ref[head] = jnp.zeros((length, HEAD_DIM), F32)
        dv_ref[head] = jnp.zeros((length, HEAD_DIM), F32)
        for first in range(0, length, rows):
            count = first + rows
            probs, query, keys = block_probs(q_ref, k_ref, head, first, rows)
            d_out = do_ref[head, first:count, :]
            d_probs = dot(d_out, v_ref[head, 0:count, :], ((1,), (1,)))
            row_dot = jnp.sum(d_probs * probs, -1, keepdims=True)
            d_scores = (probs * (d_probs - row_dot) * (HEAD_DIM**-0.5)).astype(BF16)
            dq_ref[head, first:count, :] = dot(d_scores, keys, ((1,), (0,))).astype(BF16)
            dk_ref[head, 0:count, :] += dot(d_scores, query, ((0,), (0,)))
            dv_ref[head, 0:count, :] += dot(probs.astype(BF16), d_out, ((0,), (0,)))

    for head in range(heads):
        for place, part in enumerate((dq_ref, dk_ref, dv_ref)):
            start = (place * heads + head) * HEAD_DIM
            out_ref[:, start : start + HEAD_DIM] = part[head].astype(BF16)


def attend_back(mixed, d_attended, heads):
    length = mixed.shape[0]
    part = pltpu.VMEM((heads, length, HEAD_DIM), BF16)
    wide = pltpu.VMEM((heads, length, HEAD_DIM), F32)
    return pl.pallas_call(
        attend_back_kernel,
        out_shape=jax.ShapeDtypeStruct((length, 3 * heads * HEAD_DIM), BF16),
        in_specs=[pl.BlockSpec(memory_space=pltpu.VMEM)] * 2,
        out_specs=pl.BlockSpec(memory_space=pltpu.VMEM),
        scratch_shapes=[part, part, part, part, part, wide, wide],
        name="attend_back",
    )(mixed, d_attended)


class Place:
    def __init__(self, tokens):
        self.replicas = lax.axis_size("replica")
        self.shards = lax.axis_size("shard")
        self.r = lax.axis_index("replica")
        self.s = lax.axis_index("shard")
        self.held, self.rows, self.width = tokens.shape
        self.heads = -(-HEADS // self.replicas)
        self.padded = self.heads * self.replicas
        assert self.held * self.replicas == self.shards

    def to_sequences(self, blocks):
        held = self.held
        got = []
        for turn in range(held):
            pairs = []
            for r in range(self.replicas):
                for s in range(self.shards):
                    pick = (s + turn) % held
                    target = (s // held) * self.shards + held * r + pick
                    pairs.append((r * self.shards + s, target))
            block = lax.dynamic_index_in_dim(blocks, (self.s + turn) % held, 0, keepdims=False)
            got.append(lax.ppermute(block, BOTH, pairs))
        stacked = jnp.stack(got)
        ordered = [
            lax.dynamic_index_in_dim(stacked, (self.s - u) % held, 0, keepdims=False)
            for u in range(held)
        ]
        return jnp.concatenate(ordered, 0)

    def from_sequences(self, values):
        held, rows = self.held, self.rows
        blocks = values.reshape(held, rows, values.shape[-1])
        got = []
        for turn in range(held):
            pairs = []
            for r in range(self.replicas):
                for s in range(self.shards):
                    pick = (s + turn) % held
                    target = (s // held) * self.shards + held * r + pick
                    pairs.append((target, r * self.shards + s))
            block = lax.dynamic_index_in_dim(blocks, (self.s - turn) % held, 0, keepdims=False)
            got.append(lax.ppermute(block, BOTH, pairs))
        stacked = jnp.stack(got)
        return jnp.stack(
            [
                lax.dynamic_index_in_dim(stacked, (i - self.s) % held, 0, keepdims=False)
                for i in range(held)
            ]
        )

    def to_heads(self, values):
        return lax.all_to_all(values, "replica", 1, 0, tiled=True)

    def to_rows(self, values):
        return lax.all_to_all(values, "replica", 0, 1, tiled=True)

    def mix_columns(self, weight):
        lead = weight.shape[:-1]
        parts = weight.reshape(lead + (3, HEADS, HEAD_DIM))
        extra = [(0, 0)] * len(lead) + [(0, 0), (0, self.padded - HEADS), (0, 0)]
        parts = jnp.pad(parts, extra)
        parts = parts.reshape(lead + (3, self.replicas, self.heads * HEAD_DIM))
        return jnp.swapaxes(parts, -3, -2).reshape(lead + (-1,))

    def unmix_columns(self, values):
        lead = values.shape[:-1]
        parts = values.reshape(lead + (self.replicas, 3, self.heads * HEAD_DIM))
        parts = jnp.swapaxes(parts, -3, -2).reshape(lead + (3, self.padded, HEAD_DIM))
        return parts[..., :HEADS, :].reshape(lead + (-1,))


MESH = pl.DeviceIdType.MESH


class Grid:
    def __init__(self, replicas, shards):
        self.cores = 2 if replicas % 2 == 0 else 1
        self.xs = replicas // self.cores
        self.zs = 4 if shards % 4 == 0 else 1
        self.ys = shards // self.zs
        r, s = lax.axis_index("replica"), lax.axis_index("shard")
        self.x, self.core = r // self.cores, lax.rem(r, self.cores)
        self.z, self.y = s // self.ys, lax.rem(s, self.ys)

    def device(self, x=0, core=0, z=0, y=0):
        to_x = lax.rem(self.x + x + self.xs, self.xs)
        to_core = lax.rem(self.core + core, self.cores)
        to_z = lax.rem(self.z + z + self.zs, self.zs)
        to_y = lax.rem(self.y + y + self.ys, self.ys)
        return {"replica": to_x * self.cores + to_core, "shard": to_z * self.ys + to_y}

    def block(self, z_back, y_back):
        from_z = lax.rem(self.z - z_back + self.zs, self.zs)
        from_y = lax.rem(self.y - y_back + self.ys, self.ys)
        return from_z * self.ys + from_y

    def greet(self):
        near = []
        for axis, size in (("x", self.xs), ("core", self.cores), ("z", self.zs), ("y", self.ys)):
            if size > 1:
                near.append({axis: 1})
            if size > 2:
                near.append({axis: -1})
        barrier = pltpu.get_barrier_semaphore()
        for step in near:
            pl.semaphore_signal(barrier, 1, device_id=self.device(**step), device_id_type=MESH)
        pl.semaphore_wait(barrier, len(near))


def window(ref, row, rows, col, cols):
    row = row if isinstance(row, int) else pl.multiple_of(row, 16)
    col = col if isinstance(col, int) else pl.multiple_of(col, 128)
    return ref.at[pl.ds(row, rows), pl.ds(col, cols)]


def part_of(grid, kind, ref, shape, block, x_at):
    rows, cols = shape
    row = block * rows
    if kind == "whole":
        return window(ref, row, rows, 0, cols)
    half = cols // grid.cores
    if kind == "half":
        return window(ref, row, rows, grid.core * half, half)
    if kind == "columns":
        share = half // grid.xs
        return window(ref, row, rows, grid.core * half + x_at * share, share)
    share = rows // grid.xs
    return window(ref, row + x_at * share, share, grid.core * half, half)


def half_of(grid, ref, shape, block):
    rows, cols = shape
    half = cols // grid.cores
    return window(ref, block * rows, rows, grid.core * half, half)


def copies_of_gather(kind, grid):
    blocks = grid.zs * grid.ys
    count = blocks - 1
    if kind in ("columns", "rows"):
        count += (blocks - 1) * (grid.xs - 1)
    if kind != "whole":
        count += (blocks - 1) * (grid.cores - 1)
    return count


def gather_kernel(replicas, shards, kinds, *refs):
    count = len(kinds)
    sources, targets = refs[:count], refs[count : 2 * count]
    send_sems, recv_sems, own_sems = refs[2 * count :]
    grid = Grid(replicas, shards)
    shapes = [source.shape for source in sources]
    started = []

    def send(source, target, device):
        at = len(started)
        copy = pltpu.make_async_remote_copy(
            src_ref=source,
            dst_ref=target,
            send_sem=send_sems.at[at],
            recv_sem=recv_sems.at[at],
            device_id=device,
            device_id_type=MESH,
        )
        copy.start()
        started.append(copy)
        return copy

    def fetched(job, z_back, y_back, x_back=0):
        kind, shape = kinds[job], shapes[job]
        x_at = lax.rem(grid.x - x_back + grid.xs, grid.xs)
        target = part_of(grid, kind, targets[job], shape, grid.block(z_back, y_back), x_at)
        if z_back == 0 and y_back == 0:
            return part_of(grid, kind, sources[job], shape, 0, x_at), target
        return target, target

    grid.greet()
    own = []
    for job in range(count):
        rows = shapes[job][0]
        place = targets[job].at[pl.ds(pl.multiple_of(grid.block(0, 0) * rows, 16), rows), :]
        copy = pltpu.make_async_copy(sources[job], place, own_sems.at[job])
        copy.start()
        own.append(copy)

    along_z, along_y, along_x, along_core = {}, {}, {}, {}
    for step in range(grid.zs + 3):
        for job, kind in enumerate(kinds):
            z_back = step
            if z_back < grid.zs:
                if z_back > 0:
                    along_z[job, z_back - 1].wait_recv()
                if z_back < grid.zs - 1:
                    along_z[job, z_back] = send(*fetched(job, z_back, 0), grid.device(z=1))
                if grid.ys > 1:
                    along_y[job, z_back, 0] = send(*fetched(job, z_back, 0), grid.device(y=1))
            z_back = step - 1
            if 0 <= z_back < grid.zs:
                for y_back in range(1, grid.ys):
                    along_y[job, z_back, y_back - 1].wait_recv()
                    if y_back < grid.ys - 1:
                        along_y[job, z_back, y_back] = send(
                            *fetched(job, z_back, y_back), grid.device(y=1)
                        )
                if kind in ("columns", "rows") and grid.xs > 1:
                    for y_back in range(0 if z_back else 1, grid.ys):
                        along_x[job, z_back, y_back, 0] = send(
                            *fetched(job, z_back, y_back), grid.device(x=1)
                        )
            z_back = step - 2
            if 0 <= z_back < grid.zs and kind != "whole":
                for y_back in range(0 if z_back else 1, grid.ys):
                    if kind != "half":
                        for x_back in range(1, grid.xs):
                            along_x[job, z_back, y_back, x_back - 1].wait_recv()
                            if x_back < grid.xs - 1:
                                along_x[job, z_back, y_back, x_back] = send(
                                    *fetched(job, z_back, y_back, x_back), grid.device(x=1)
                                )
                    if grid.cores > 1:
                        half = half_of(grid, targets[job], shapes[job], grid.block(z_back, y_back))
                        along_core[job, z_back, y_back] = send(half, half, grid.device(core=1))
            z_back = step - 3
            if 0 <= z_back < grid.zs and kind != "whole" and grid.cores > 1:
                for y_back in range(0 if z_back else 1, grid.ys):
                    along_core[job, z_back, y_back].wait_recv()
    for copy in started:
        copy.wait_send()
    for copy in own:
        copy.wait()


def gather_shards(place, kinds, shards):
    sizes = Grid(place.replicas, place.shards)
    copies = sum(copies_of_gather(kind, sizes) for kind in kinds)
    return pl.pallas_call(
        functools.partial(gather_kernel, place.replicas, place.shards, kinds),
        out_shape=[
            jax.ShapeDtypeStruct((place.shards * a.shape[0], a.shape[1]), a.dtype) for a in shards
        ],
        in_specs=[pl.BlockSpec(memory_space=pltpu.VMEM)] * len(shards),
        out_specs=[pl.BlockSpec(memory_space=pl.ANY)] * len(shards),
        scratch_shapes=[
            pltpu.SemaphoreType.DMA((copies,)),
            pltpu.SemaphoreType.DMA((copies,)),
            pltpu.SemaphoreType.DMA((len(shards),)),
        ],
        compiler_params=pltpu.CompilerParams(collective_id=0, has_side_effects=True),
        name="gather_shards",
    )(*shards)


def gather_all(place, vectors, mix, out_w, up, down):
    layers = mix.shape[0]
    packed = jnp.concatenate(vectors, -1).reshape(-1)
    size = packed.shape[0]
    lanes = 128 * -(-size // (16 * 128))
    packed = jnp.pad(packed, (0, 16 * lanes - size)).reshape(16, lanes)
    first = jnp.concatenate([mix, out_w], -1)
    kinds, shards = ["whole"], [packed]
    for layer in range(layers):
        kinds += ["half", "columns", "rows"]
        shards += [first[layer], up[layer], down[layer]]
    whole = gather_shards(place, tuple(kinds), shards)
    flat = whole[0].reshape(place.shards, -1)[:, :size].reshape(place.shards, layers, -1)
    out, start = [], 0
    for vector in vectors:
        piece = flat[:, :, start : start + vector.shape[1]]
        out.append(jnp.swapaxes(piece, 0, 1).reshape(layers, -1).astype(F32))
        start += vector.shape[1]
    return [whole[1 + 3 * n : 4 + 3 * n] for n in range(layers)], out


class Copies:
    def __init__(self, send_sems, recv_sems):
        self.send_sems, self.recv_sems, self.started = send_sems, recv_sems, []

    def send(self, source, target, device):
        at = len(self.started)
        copy = pltpu.make_async_remote_copy(
            src_ref=source,
            dst_ref=target,
            send_sem=self.send_sems.at[at],
            recv_sem=self.recv_sems.at[at],
            device_id=device,
            device_id_type=MESH,
        )
        copy.start()
        self.started.append(copy)
        return copy

    def finish(self):
        for copy in self.started:
            copy.wait_send()


def by_rows(rows, body):
    @pl.loop(0, rows // 16)
    def _(at):
        body(pl.ds(pl.multiple_of(at * 16, 16), 16))


def share_of(kind, grid, rows, cols):
    if kind == "columns":
        return rows, cols // grid.xs
    if kind == "rows":
        return rows // grid.xs, cols
    return rows, cols


def x_window(kind, ref, shape, x_at):
    rows, cols = shape
    lead = (slice(None),) * (len(ref.shape) - 2)
    if kind == "columns":
        return ref.at[lead + (slice(None), pl.ds(pl.multiple_of(x_at * cols, 128), cols))]
    return ref.at[lead + (pl.ds(pl.multiple_of(x_at * rows, 16), rows), slice(None))]


def reduce_kernel(replicas, shards, jobs, *refs):
    kinds = [kind for kind, _, _ in jobs]
    count = len(jobs)
    outputs = 1 + max(out for _, out, _ in jobs)
    grid = Grid(replicas, shards)
    zs, ys, xs = grid.zs, grid.ys, grid.xs
    refs = list(refs)

    def take(number):
        taken = refs[:number]
        del refs[:number]
        return taken

    grads, (vec_ref,), outs, (vec_out,) = take(count), take(1), take(outputs), take(1)
    own, got, x_got, y_got, z_got, x_sum, done = (take(count) for _ in range(7))
    vec_got, vec_sum, send_sems, recv_sems, own_sems = refs
    copies = Copies(send_sems, recv_sems)
    r, s = lax.axis_index("replica"), lax.axis_index("shard")
    halves = [(g.shape[1], g.shape[2] // grid.cores) for g in grads]
    shares = [share_of(kind, grid, *half) for kind, half in zip(kinds, halves)]

    barrier = pltpu.get_barrier_semaphore()
    for step in range(1, shards):
        peer = {"replica": r, "shard": lax.rem(s + step, shards)}
        pl.semaphore_signal(barrier, 1, device_id=peer, device_id_type=MESH)
    for step in range(1, replicas):
        peer = {"replica": lax.rem(r + step, replicas), "shard": s}
        pl.semaphore_signal(barrier, 1, device_id=peer, device_id_type=MESH)
    pl.semaphore_wait(barrier, shards + replicas - 2)

    def target_z(t):
        return lax.rem(grid.z + 2 * zs - 1 - t, zs)

    def load(job, t):
        half = halves[job][1]
        copy = pltpu.make_async_copy(
            grads[job].at[
                pl.ds(target_z(t) * ys, ys),
                :,
                pl.ds(pl.multiple_of(grid.core * half, 128), half),
            ],
            own[job].at[t % 2],
            own_sems.at[job, t % 2],
        )
        copy.start()
        return copy

    loads, by_core = {}, {}
    for t in range(zs):
        for job in range(count):
            half = halves[job][1]
            other = lax.rem(grid.core + 1, grid.cores)
            by_core[job, t] = copies.send(
                grads[job].at[
                    pl.ds(target_z(t) * ys, ys), :, pl.ds(pl.multiple_of(other * half, 128), half)
                ],
                got[job].at[t],
                grid.device(core=1),
            )
            if t < 2:
                loads[job, t] = load(job, t)
    vec_copies = []
    for step in range(1, shards):
        to = lax.rem(s + step, shards)
        vec_copies.append(
            copies.send(vec_ref.at[to], vec_got.at[step - 1], {"replica": r, "shard": to})
        )

    by_x, by_y, by_z = {}, {}, {}

    def base(job, t):
        return got[job].at[t] if kinds[job] == "half" else x_got[job].at[t, 0]

    def send_y(job, t):
        for step in range(1, ys):
            by_y[job, t, step] = copies.send(
                base(job, t).at[lax.rem(grid.y + step, ys)],
                y_got[job].at[t, step - 1],
                grid.device(y=step),
            )

    for step in range(zs + 4):
        for job, kind in enumerate(kinds):
            rows, cols = shares[job]
            t = step
            if t < zs:
                loads[job, t].wait()
                by_core[job, t].wait_recv()
                for y in range(ys):
                    mine, sums = own[job].at[t % 2, y], got[job].at[t, y]

                    def both(at, mine=mine, sums=sums):
                        sums[at] = (mine[at].astype(F32) + sums[at].astype(F32)).astype(BF16)

                    by_rows(halves[job][0], both)
                if t + 2 < zs:
                    loads[job, t + 2] = load(job, t + 2)
                if kind == "half":
                    send_y(job, t)
                else:
                    for turn in range(1, xs):
                        by_x[job, t, turn] = copies.send(
                            x_window(kind, got[job].at[t], shares[job], lax.rem(grid.x + turn, xs)),
                            x_got[job].at[t, turn - 1],
                            grid.device(x=turn),
                        )
            t = step - 1
            if 0 <= t < zs and kind != "half":
                for turn in range(1, xs):
                    by_x[job, t, turn].wait_recv()
                for y in range(ys):
                    mine = x_window(kind, got[job].at[t, y], shares[job], grid.x)
                    parts = [x_got[job].at[t, turn, y] for turn in range(xs - 1)]

                    def all_x(at, mine=mine, parts=parts):
                        total = mine[at].astype(F32)
                        for part in parts:
                            total += part[at].astype(F32)
                        parts[0][at] = total.astype(BF16)

                    by_rows(rows, all_x)
                send_y(job, t)
            t = step - 2
            if 0 <= t < zs:
                for turn in range(1, ys):
                    by_y[job, t, turn].wait_recv()
                parts = [y_got[job].at[t, turn] for turn in range(ys - 1)]
                target = parts[0]
                if t > 0:
                    by_z[job, t - 1].wait_recv()
                    parts.append(z_got[job].at[t - 1])
                if t == zs - 1:
                    target = (
                        x_sum[job].at[grid.x]
                        if kind == "half"
                        else x_window(kind, done[job].at[0], shares[job], grid.x)
                    )
                mine = base(job, t).at[grid.y]

                def all_y(at, mine=mine, parts=parts, target=target):
                    total = mine[at].astype(F32)
                    for part in parts:
                        total += part[at].astype(F32)
                    target[at] = total.astype(BF16)

                by_rows(rows, all_y)
                if t < zs - 1:
                    by_z[job, t] = copies.send(target, z_got[job].at[t], grid.device(z=1))
                else:
                    for turn in range(1, xs):
                        by_x[job, "done", turn] = copies.send(target, target, grid.device(x=turn))
            if step == zs + 2:
                for turn in range(1, xs):
                    by_x[job, "done", turn].wait_recv()
                if kind == "half":
                    sums, target = x_sum[job], done[job].at[0]

                    def across(at, sums=sums, target=target):
                        total = sums[0, at].astype(F32)
                        for x_at in range(1, xs):
                            total += sums[x_at, at].astype(F32)
                        target[at] = total.astype(BF16)

                    by_rows(rows, across)
                by_core[job, "done"] = copies.send(
                    done[job].at[0], done[job].at[1], grid.device(core=1)
                )
            if step == zs + 3:
                by_core[job, "done"].wait_recv()
                half_rows, half = halves[job]
                _, out, layer = jobs[job]
                for side in range(2):
                    column = lax.rem(grid.core + side, 2) * half
                    place = outs[out].at[layer, :, pl.ds(pl.multiple_of(column, 128), half)]

                    def write(at, place=place, source=done[job].at[side]):
                        place[at] = source[at].astype(F32)

                    by_rows(half_rows, write)

        if step == zs + 1:
            total = vec_ref[s]
            for copy in vec_copies:
                copy.wait_recv()
            for at in range(shards - 1):
                total += vec_got[at]
            vec_sum[r] = total
            vec_copies = [
                copies.send(
                    vec_sum.at[r],
                    vec_sum.at[r],
                    {"replica": lax.rem(r + turn, replicas), "shard": s},
                )
                for turn in range(1, replicas)
            ]
        if step == zs + 3:
            for copy in vec_copies:
                copy.wait_recv()
            total = vec_sum[0]
            for at in range(1, replicas):
                total += vec_sum[at]
            vec_out[...] = total
    copies.finish()


def reduce_all(place, grads, vectors):
    grid = Grid(place.replicas, place.shards)
    zs, ys, xs = grid.zs, grid.ys, grid.xs
    layers, members = len(grads), len(grads[0])
    jobs, arrays = [], []
    for layer in reversed(range(layers)):
        for out, (kind, value) in enumerate(grads[layer]):
            jobs.append((kind, out, layer))
            arrays.append(value.reshape(place.shards, -1, value.shape[1]))
    own, got, x_got, y_got, z_got, x_sum, done = ([] for _ in range(7))
    copies = (place.shards - 1) + (place.replicas - 1)
    for (kind, _, _), value in zip(jobs, arrays):
        rows, half = value.shape[1], value.shape[2] // grid.cores
        share = share_of(kind, grid, rows, half)
        split = kind != "half"
        tiny = (16, 128)
        own.append(pltpu.VMEM((2, ys, rows, half), BF16))
        got.append(pltpu.VMEM((zs, ys, rows, half), BF16))
        x_got.append(pltpu.VMEM((zs, xs - 1, ys) + share if split else tiny, BF16))
        y_got.append(pltpu.VMEM((zs, ys - 1) + share, BF16))
        z_got.append(pltpu.VMEM((zs - 1,) + share, BF16))
        x_sum.append(pltpu.VMEM(tiny if split else (xs,) + share, BF16))
        done.append(pltpu.VMEM((2, rows, half), BF16))
        copies += zs + (zs * (xs - 1) if split else 0) + zs * (ys - 1) + (zs - 1) + (xs - 1) + 1
    shapes = [
        jax.ShapeDtypeStruct((layers, arrays[m].shape[1], arrays[m].shape[2]), F32)
        for m in range(members)
    ]
    vec = vectors.shape[1:]
    return pl.pallas_call(
        functools.partial(reduce_kernel, place.replicas, place.shards, tuple(jobs)),
        out_shape=shapes + [jax.ShapeDtypeStruct(vec, F32)],
        in_specs=[pl.BlockSpec(memory_space=pl.ANY)] * len(arrays)
        + [pl.BlockSpec(memory_space=pltpu.VMEM)],
        out_specs=[pl.BlockSpec(memory_space=pltpu.VMEM)] * (members + 1),
        scratch_shapes=own
        + got
        + x_got
        + y_got
        + z_got
        + x_sum
        + done
        + [
            pltpu.VMEM((place.shards - 1,) + vec, F32),
            pltpu.VMEM((place.replicas,) + vec, F32),
            pltpu.SemaphoreType.DMA((copies,)),
            pltpu.SemaphoreType.DMA((copies,)),
            pltpu.SemaphoreType.DMA((len(jobs), 2)),
        ],
        compiler_params=pltpu.CompilerParams(
            collective_id=1, has_side_effects=True, vmem_limit_bytes=60 * 1024 * 1024
        ),
        name="reduce_all",
    )(*arrays, vectors)


def pack_vectors(place, by_layer):
    sizes = [vector.shape[0] // place.shards for vector in by_layer[0]]
    packed = jnp.concatenate(
        [vector.reshape(place.shards, -1) for vectors in by_layer for vector in vectors], 1
    )
    size = packed.shape[1]
    lanes = 128 * -(-size // (16 * 128))
    packed = jnp.pad(packed, ((0, 0), (0, 16 * lanes - size)))
    return packed.reshape(place.shards, 16, lanes), sizes


def unpack_vectors(summed, layers, sizes):
    flat = summed.reshape(-1)[: layers * sum(sizes)].reshape(layers, -1)
    out, start = [], 0
    for size in sizes:
        out.append(flat[:, start : start + size])
        start += size
    return out


def forward_block(place, current, weights, vectors):
    mix_out, up, down = weights
    mix, out_w = jnp.split(mix_out, [mix_out.shape[1] - place.width], 1)
    gain_one, shift_one, mix_bias, out_bias, gain_two, shift_two, up_bias, down_bias = vectors
    normed = norm_rows(current, gain_one, shift_one).astype(BF16)
    mixed = (dot(normed, mix, ((1,), (0,))) + mix_bias).astype(BF16)
    mixed = place.to_heads(mixed)
    attended = place.to_rows(attend(mixed, place.heads))[:, : place.width]
    x_mid = current + (dot(attended, out_w, ((1,), (0,))) + out_bias)
    moved = norm_rows(x_mid, gain_two, shift_two).astype(BF16)
    pre = dot(moved, up, ((1,), (0,))) + up_bias
    act = jax.nn.gelu(pre, approximate=True).astype(BF16)
    result = x_mid + dot(act, down, ((1,), (0,))) + down_bias
    return result, (current, normed, mixed, attended, x_mid, moved, pre, act)


def backward_block(place, grad_next, weights, vectors, saved):
    mix_out, up, down = weights
    mix, out_w = jnp.split(mix_out, [mix_out.shape[1] - place.width], 1)
    gain_one, shift_one, mix_bias, out_bias, gain_two, shift_two, up_bias, down_bias = vectors
    current, normed, mixed, attended, x_mid, moved, pre, act = saved
    d_ffn = grad_next.astype(BF16)
    grad_down = dot(act, d_ffn, ((0,), (0,))).astype(BF16)
    grad_b_down = jnp.sum(d_ffn.astype(F32), 0)
    d_act = dot(d_ffn, down, ((1,), (1,)))
    gelu_back = jax.vjp(lambda inner: jax.nn.gelu(inner, approximate=True), pre)[1]
    d_pre = gelu_back(d_act)[0].astype(BF16)
    grad_up = dot(moved, d_pre, ((0,), (0,))).astype(BF16)
    grad_b_up = jnp.sum(d_pre.astype(F32), 0)
    d_moved = dot(d_pre, up, ((1,), (1,)))
    norm_back = jax.vjp(norm_rows, x_mid, gain_two, shift_two)[1]
    d_from_norm, grad_gain_two, grad_shift_two = norm_back(d_moved)
    grad_mid = grad_next + d_from_norm
    d_branch = grad_mid.astype(BF16)
    grad_out = dot(attended, d_branch, ((0,), (0,))).astype(BF16)
    grad_b_out = jnp.sum(d_branch.astype(F32), 0)
    d_att = dot(d_branch, out_w, ((1,), (1,))).astype(BF16)
    d_att = jnp.pad(d_att, ((0, 0), (0, place.padded * HEAD_DIM - place.width)))
    d_mixed = place.to_rows(attend_back(mixed, place.to_heads(d_att), place.heads))
    grad_mix = dot(normed, d_mixed, ((0,), (0,))).astype(BF16)
    grad_b_mix = place.unmix_columns(jnp.sum(d_mixed.astype(F32), 0))
    grad_b_query = grad_b_mix[: place.width]
    grad_b_value = grad_b_mix[2 * place.width :]
    d_normed = dot(d_mixed, mix, ((1,), (1,)))
    first_back = jax.vjp(norm_rows, current, gain_one, shift_one)[1]
    d_from_first, grad_gain_one, grad_shift_one = first_back(d_normed)
    grad_current = grad_mid + d_from_first
    grad_vectors = (
        grad_gain_one,
        grad_shift_one,
        grad_b_query,
        grad_b_value,
        grad_b_out,
        grad_gain_two,
        grad_shift_two,
        grad_b_up,
        grad_b_down,
    )
    return grad_current, (grad_mix, grad_out, grad_up, grad_down), grad_vectors


def per_device(
    tokens,
    gain_one,
    shift_one,
    query_key_value_weight,
    b_query,
    b_value,
    output_weight,
    output_proj_bias,
    gain_two,
    shift_two,
    up_weight,
    up_bias,
    down_weight,
    down_bias,
    cotangent,
):
    place = Place(tokens)
    layers = gain_one.shape[0]
    mix_weight = place.mix_columns(query_key_value_weight)
    weights, vectors = gather_all(
        place,
        (
            gain_one,
            shift_one,
            b_query,
            b_value,
            output_proj_bias,
            gain_two,
            shift_two,
            up_bias,
            down_bias,
        ),
        mix_weight,
        output_weight,
        up_weight,
        down_weight,
    )
    g1, s1, bq, bv, bo, g2, s2, bu, bd = vectors
    mix_bias = place.mix_columns(jnp.concatenate([bq, jnp.zeros_like(bq), bv], -1))

    def layer_vectors(n):
        return (g1[n], s1[n], mix_bias[n], bo[n], g2[n], s2[n], bu[n], bd[n])

    current = place.to_sequences(tokens).astype(F32)
    saved = []
    for n in range(layers):
        current, kept = forward_block(place, current, weights[n], layer_vectors(n))
        saved.append(kept)
    output = place.from_sequences(current.astype(BF16))
    grad_now = place.to_sequences(cotangent).astype(F32)
    weight_grads, vector_grads = [None] * layers, [None] * layers
    for n in reversed(range(layers)):
        grad_now, local, vector_grads[n] = backward_block(
            place, grad_now, weights[n], layer_vectors(n), saved[n]
        )
        weight_grads[n] = list(zip(("half", "half", "columns", "rows"), local))
    grad_tokens = place.from_sequences(grad_now.astype(BF16)).astype(F32)
    packed, sizes = pack_vectors(place, vector_grads)
    grad_mix, grad_out, grad_up, grad_down, summed = reduce_all(place, weight_grads, packed)
    grad_mix = place.unmix_columns(grad_mix)
    own = unpack_vectors(summed, layers, sizes)
    (
        grad_gain_one,
        grad_shift_one,
        grad_b_query,
        grad_b_value,
        grad_b_out,
        grad_gain_two,
        grad_shift_two,
        grad_b_up,
        grad_b_down,
    ) = own
    return (
        output,
        grad_tokens,
        grad_gain_one,
        grad_shift_one,
        grad_mix,
        grad_b_query,
        grad_b_value,
        grad_out,
        grad_b_out,
        grad_gain_two,
        grad_shift_two,
        grad_up,
        grad_b_up,
        grad_down,
        grad_b_down,
    )


def solution(mesh):
    vector, matrix = P(None, "shard"), P(None, "shard", None)
    rows = P("replica", "shard", None)
    in_specs = (
        rows,
        vector,
        vector,
        matrix,
        vector,
        vector,
        matrix,
        vector,
        vector,
        vector,
        matrix,
        vector,
        matrix,
        vector,
        rows,
    )
    out_specs = (
        rows,
        rows,
        vector,
        vector,
        matrix,
        vector,
        vector,
        matrix,
        vector,
        vector,
        vector,
        matrix,
        vector,
        matrix,
        vector,
    )
    return jax.shard_map(
        per_device, mesh=mesh, in_specs=in_specs, out_specs=out_specs, check_vma=False
    )
```

```python
import functools

import jax
import jax.numpy as jnp
from jax import lax
from jax.experimental import pallas as pl
from jax.experimental.pallas import tpu as pltpu
from jax.sharding import PartitionSpec as P

HEADS = 12
HEAD_DIM = 64
EPSILON = 1e-05
MASKED = -1e30
F32 = jnp.float32
BF16 = jnp.bfloat16
BOTH = ("replica", "shard")
MESH = pl.DeviceIdType.MESH
VMEM_BLOCK = pl.BlockSpec(memory_space=pltpu.VMEM)
ANY_BLOCK = pl.BlockSpec(memory_space=pl.ANY)


def dot(a, b, contract):
    return lax.dot_general(a, b, (contract, ((), ())), preferred_element_type=F32)


def norm_rows(values, gain, shift):
    centre = values - jnp.mean(values, -1, keepdims=True)
    spread = jnp.mean(centre * centre, -1, keepdims=True)
    return centre * lax.rsqrt(spread + EPSILON) * gain + shift


class Place:
    def __init__(self, replicas, shards):
        self.replicas, self.shards = replicas, shards
        self.cores = 2
        self.xs = replicas // self.cores
        self.zs = 4
        self.ys = shards // self.zs
        assert self.xs * self.cores == replicas and self.zs * self.ys == shards
        self.heads = -(-HEADS // replicas)
        self.padded = self.heads * replicas
        self.span = 3 * self.heads * HEAD_DIM
        self.columns = 128 * -(-self.span // 128)

    def locate(self):
        self.r, self.s = lax.axis_index("replica"), lax.axis_index("shard")
        self.x, self.core = self.r // self.cores, lax.rem(self.r, self.cores)
        self.z, self.y = self.s // self.ys, lax.rem(self.s, self.ys)
        return self

    def device(self, x=0, core=0, z=0, y=0):
        to_x = lax.rem(self.x + x + self.xs, self.xs)
        to_core = lax.rem(self.core + core, self.cores)
        to_z = lax.rem(self.z + z + self.zs, self.zs)
        to_y = lax.rem(self.y + y + self.ys, self.ys)
        return {"replica": to_x * self.cores + to_core, "shard": to_z * self.ys + to_y}

    def block(self, z_back, y_back):
        from_z = lax.rem(self.z - z_back + self.zs, self.zs)
        from_y = lax.rem(self.y - y_back + self.ys, self.ys)
        return from_z * self.ys + from_y

    def turn_pairs(self, turn, held):
        pairs = []
        for r in range(self.replicas):
            for s in range(self.shards):
                target = (s // held) * self.shards + held * r + (s + turn) % held
                pairs.append((r * self.shards + s, target))
        return pairs

    def to_sequences(self, blocks):
        held = blocks.shape[0]
        assert held * self.replicas == self.shards
        got = []
        for turn in range(held):
            block = lax.dynamic_index_in_dim(blocks, (self.s + turn) % held, 0, keepdims=False)
            got.append(lax.ppermute(block, BOTH, self.turn_pairs(turn, held)))
        stacked = jnp.stack(got)
        ordered = [
            lax.dynamic_index_in_dim(stacked, (self.s - u) % held, 0, keepdims=False)
            for u in range(held)
        ]
        return jnp.concatenate(ordered, 0)

    def from_sequences(self, values, held):
        blocks = values.reshape(held, -1, values.shape[-1])
        got = []
        for turn in range(held):
            pairs = [(b, a) for a, b in self.turn_pairs(turn, held)]
            block = lax.dynamic_index_in_dim(blocks, (self.s - turn) % held, 0, keepdims=False)
            got.append(lax.ppermute(block, BOTH, pairs))
        stacked = jnp.stack(got)
        return jnp.stack(
            [
                lax.dynamic_index_in_dim(stacked, (i - self.s) % held, 0, keepdims=False)
                for i in range(held)
            ]
        )

    def mix_columns(self, weight):
        lead = weight.shape[:-1]
        parts = weight.reshape(lead + (3, HEADS, HEAD_DIM))
        extra = [(0, 0)] * len(lead) + [(0, 0), (0, self.padded - HEADS), (0, 0)]
        parts = jnp.pad(parts, extra)
        parts = parts.reshape(lead + (3, self.replicas, self.heads * HEAD_DIM))
        parts = jnp.swapaxes(parts, -3, -2).reshape(lead + (self.replicas, self.span))
        parts = jnp.pad(parts, [(0, 0)] * (len(lead) + 1) + [(0, self.columns - self.span)])
        return parts.reshape(lead + (-1,))

    def unmix_columns(self, values):
        lead = values.shape[:-1]
        parts = values.reshape(lead + (self.replicas, self.columns))[..., : self.span]
        parts = parts.reshape(lead + (self.replicas, 3, self.heads * HEAD_DIM))
        parts = jnp.swapaxes(parts, -3, -2).reshape(lead + (3, self.padded, HEAD_DIM))
        return parts[..., :HEADS, :].reshape(lead + (-1,))


class Copies:
    def __init__(self, send_sems, recv_sems):
        self.send_sems, self.recv_sems, self.started = send_sems, recv_sems, []

    def send(self, source, target, device):
        at = len(self.started)
        copy = pltpu.make_async_remote_copy(
            src_ref=source,
            dst_ref=target,
            send_sem=self.send_sems.at[at],
            recv_sem=self.recv_sems.at[at],
            device_id=device,
            device_id_type=MESH,
        )
        copy.start()
        self.started.append(copy)
        return copy

    def finish(self):
        for copy in self.started:
            copy.wait_send()


class Task:
    def __init__(self, run, inputs, outputs, scratch, copies):
        self.run, self.inputs, self.outputs = run, inputs, outputs
        self.scratch, self.copies = scratch, copies


def fuse(place, name, collective_id, tasks, order):
    sizes = (place.replicas, place.shards)
    count = sum(task.copies for task in tasks)

    def kernel(*refs):
        here = Place(*sizes).locate()
        refs = list(refs)

        def take(number):
            taken = refs[:number]
            del refs[:number]
            return taken

        ins = [take(len(task.inputs)) for task in tasks]
        outs = [take(len(task.outputs)) for task in tasks]
        own = [take(len(task.scratch)) for task in tasks]
        copies = Copies(*refs)
        barrier = pltpu.get_barrier_semaphore()
        for step in range(1, here.shards):
            peer = {"replica": here.r, "shard": lax.rem(here.s + step, here.shards)}
            pl.semaphore_signal(barrier, 1, device_id=peer, device_id_type=MESH)
        for step in range(1, here.replicas):
            peer = {"replica": lax.rem(here.r + step, here.replicas), "shard": here.s}
            pl.semaphore_signal(barrier, 1, device_id=peer, device_id_type=MESH)
        pl.semaphore_wait(barrier, here.shards + here.replicas - 2)
        streams = [
            task.run(here, copies, *group) for task, *group in zip(tasks, ins, outs, own)
        ]
        for at in order:
            next(streams[at], None)
        for stream in streams:
            for _ in stream:
                pass
        copies.finish()

    results = pl.pallas_call(
        kernel,
        out_shape=[shape for task in tasks for shape, _ in task.outputs],
        in_specs=[spec for task in tasks for _, spec in task.inputs],
        out_specs=[spec for task in tasks for _, spec in task.outputs],
        scratch_shapes=[shape for task in tasks for shape in task.scratch]
        + [pltpu.SemaphoreType.DMA((count,)), pltpu.SemaphoreType.DMA((count,))],
        compiler_params=pltpu.CompilerParams(
            collective_id=collective_id,
            has_side_effects=True,
            vmem_limit_bytes=60 * 1024 * 1024,
        ),
        name=name,
    )(*[value for task in tasks for value, _ in task.inputs])
    split, start = [], 0
    for task in tasks:
        split.append(list(results[start : start + len(task.outputs)]))
        start += len(task.outputs)
    return split


def by_rows(rows, body):
    @pl.loop(0, rows // 16)
    def _(at):
        body(pl.ds(pl.multiple_of(at * 16, 16), 16))


def block_probs(q_ref, k_ref, head, first, rows):
    count = first + rows
    query = q_ref[head, first:count, :]
    keys = k_ref[head, 0:count, :]
    scores = dot(query, keys, ((1,), (1,))) * (HEAD_DIM**-0.5)
    row = lax.broadcasted_iota(jnp.int32, (rows, count), 0) + first
    col = lax.broadcasted_iota(jnp.int32, (rows, count), 1)
    scores = jnp.where(row >= col, scores, MASKED)
    expo = jnp.exp(scores - jnp.max(scores, -1, keepdims=True))
    return expo / jnp.sum(expo, -1, keepdims=True), query, keys


def split_heads(source, targets):
    for place, target in enumerate(targets):
        heads = target.shape[0]
        for head in range(heads):
            start = (place * heads + head) * HEAD_DIM
            target[head] = source[:, start : start + HEAD_DIM]


class Blocks:
    def __init__(self, here, ready, land, send_sems, recv_sems):
        self.here, self.ready, self.land = here, ready, land
        self.send_sems, self.recv_sems = send_sems, recv_sems

    def copy(self, at, source):
        here = self.here
        return pltpu.make_async_remote_copy(
            src_ref=self.ready.at[at],
            dst_ref=self.land(source),
            send_sem=self.send_sems.at[at],
            recv_sem=self.recv_sems.at[source],
            device_id={"replica": at, "shard": here.s},
            device_id_type=MESH,
        )

    def send(self, at):
        here = self.here

        @pl.when(here.r != at)
        def _():
            self.copy(at, here.r).start()

        @pl.when(here.r == at)
        def _():
            self.land(at)[...] = self.ready[at]

    def finish(self):
        for at in range(self.here.replicas):

            @pl.when(self.here.r != at)
            def _(at=at):
                self.copy(at, at).wait_recv()
                self.copy(at, at).wait_send()


def attend_task(place, mixed):
    rows, replicas, heads, columns = mixed.shape[0], place.replicas, place.heads, place.columns
    length, wide = rows * replicas, heads * HEAD_DIM

    def run(here, copies, ins, outs, scratch):
        (mixed_ref,), (seq_ref, out_ref) = ins, outs
        q_ref, k_ref, v_ref, o_ref, ready, landed, send_sems, recv_sems = scratch
        mine = pl.ds(pl.multiple_of(here.r * rows, 16), rows)
        arriving = []
        for step in range(1, replicas):
            to = lax.rem(here.r + step, replicas)
            source = mixed_ref.at[:, pl.ds(pl.multiple_of(to * columns, 128), columns)]
            device = {"replica": to, "shard": here.s}
            arriving.append(copies.send(source, seq_ref.at[mine, :], device))
        seq_ref[mine, :] = mixed_ref[:, pl.ds(pl.multiple_of(here.r * columns, 128), columns)]
        yield
        for copy in arriving:
            copy.wait_recv()
        split_heads(seq_ref, (q_ref, k_ref, v_ref))
        blocks = Blocks(here, ready, lambda at: landed.at[at], send_sems, recv_sems)
        yield
        for at in range(replicas):
            first = at * rows

            @pl.loop(0, heads)
            def _(head, first=first):
                probs, _, _ = block_probs(q_ref, k_ref, head, first, rows)
                keys = v_ref[head, 0 : first + rows, :]
                o_ref[head] = dot(probs.astype(BF16), keys, ((1,), (0,))).astype(BF16)

            for head in range(heads):
                ready[at, :, head * HEAD_DIM : (head + 1) * HEAD_DIM] = o_ref[head]
            blocks.send(at)
            yield
        blocks.finish()
        width = out_ref.shape[1]
        for at in range(replicas):
            start = at * wide
            size = min(wide, width - start)
            if size > 0:
                out_ref[:, start : start + size] = landed[at, :, :size]

    part = pltpu.VMEM((heads, length, HEAD_DIM), BF16)
    return Task(
        run,
        [(mixed, VMEM_BLOCK)],
        [
            (jax.ShapeDtypeStruct((length, columns), BF16), VMEM_BLOCK),
            (jax.ShapeDtypeStruct((rows, HEADS * HEAD_DIM), BF16), VMEM_BLOCK),
        ],
        [part] * 3
        + [pltpu.VMEM((heads, rows, HEAD_DIM), BF16)]
        + [pltpu.VMEM((replicas, rows, wide), BF16)] * 2
        + [pltpu.SemaphoreType.DMA((replicas,))] * 2,
        replicas - 1,
    )


def attend_back_task(place, seq, d_attended):
    rows, width = d_attended.shape
    replicas, heads, columns = place.replicas, place.heads, place.columns
    length, wide = rows * replicas, heads * HEAD_DIM

    def run(here, copies, ins, outs, scratch):
        (seq_ref, d_ref), (out_ref,) = ins, outs
        q_ref, k_ref, v_ref, do_ref, dq_ref, dk_ref, dv_ref = scratch[:7]
        d_ready, d_landed, ready, send_sems, recv_sems = scratch[7:]
        for at in range(replicas):
            start = at * wide
            size = max(0, min(wide, width - start))
            if size > 0:
                d_ready[at, :, :size] = d_ref[:, start : start + size]
            if size < wide:
                d_ready[at, :, size:] = jnp.zeros((rows, wide - size), BF16)
        arriving = []
        for step in range(1, replicas):
            to = lax.rem(here.r + step, replicas)
            device = {"replica": to, "shard": here.s}
            arriving.append(copies.send(d_ready.at[to], d_landed.at[here.r], device))
        d_landed[here.r] = d_ready[here.r]
        yield
        split_heads(seq_ref, (q_ref, k_ref, v_ref))
        dk_ref[...] = jnp.zeros((heads, length, HEAD_DIM), F32)
        dv_ref[...] = jnp.zeros((heads, length, HEAD_DIM), F32)
        for copy in arriving:
            copy.wait_recv()
        for at in range(replicas):
            for head in range(heads):
                do_ref[head, at * rows : (at + 1) * rows, :] = d_landed[
                    at, :, head * HEAD_DIM : (head + 1) * HEAD_DIM
                ]

        def land(source):
            return out_ref.at[:, pl.ds(pl.multiple_of(source * columns, 128), columns)]

        blocks = Blocks(here, ready, land, send_sems, recv_sems)
        yield
        for at in reversed(range(replicas)):
            first = at * rows
            count = first + rows

            @pl.loop(0, heads)
            def _(head, first=first, count=count):
                probs, query, keys = block_probs(q_ref, k_ref, head, first, rows)
                d_out = do_ref[head, first:count, :]
                d_probs = dot(d_out, v_ref[head, 0:count, :], ((1,), (1,)))
                row_dot = jnp.sum(d_probs * probs, -1, keepdims=True)
                d_scores = (probs * (d_probs - row_dot) * (HEAD_DIM**-0.5)).astype(BF16)
                dq_ref[head] = dot(d_scores, keys, ((1,), (0,))).astype(BF16)
                dk_ref[head, 0:count, :] += dot(d_scores, query, ((0,), (0,)))
                dv_ref[head, 0:count, :] += dot(probs.astype(BF16), d_out, ((0,), (0,)))

            for head in range(heads):
                pieces = (
                    dq_ref[head],
                    dk_ref[head, first:count, :].astype(BF16),
                    dv_ref[head, first:count, :].astype(BF16),
                )
                for part, piece in enumerate(pieces):
                    start = (part * heads + head) * HEAD_DIM
                    ready[at, :, start : start + HEAD_DIM] = piece
            if place.span < columns:
                ready[at, :, place.span :] = jnp.zeros((rows, columns - place.span), BF16)
            blocks.send(at)
            yield
        blocks.finish()

    part = pltpu.VMEM((heads, length, HEAD_DIM), BF16)
    sums = pltpu.VMEM((heads, length, HEAD_DIM), F32)
    return Task(
        run,
        [(seq, VMEM_BLOCK), (d_attended, VMEM_BLOCK)],
        [(jax.ShapeDtypeStruct((rows, replicas * columns), BF16), VMEM_BLOCK)],
        [part] * 4
        + [pltpu.VMEM((heads, rows, HEAD_DIM), BF16), sums, sums]
        + [pltpu.VMEM((replicas, rows, wide), BF16)] * 2
        + [pltpu.VMEM((replicas, rows, columns), BF16)]
        + [pltpu.SemaphoreType.DMA((replicas,))] * 2,
        replicas - 1,
    )


def fits(place, kind, shape):
    rows, half = shape[0], shape[1] // place.cores
    if kind == "columns" and half % (128 * place.xs):
        return "half"
    if kind == "rows" and rows % (16 * place.xs):
        return "half"
    return kind


def window(ref, row, rows, col, cols):
    row = row if isinstance(row, int) else pl.multiple_of(row, 16)
    col = col if isinstance(col, int) else pl.multiple_of(col, 128)
    return ref.at[pl.ds(row, rows), pl.ds(col, cols)]


def part_of(here, kind, ref, shape, block, x_at):
    rows, cols = shape
    row = block * rows
    if kind == "whole":
        return window(ref, row, rows, 0, cols)
    half = cols // here.cores
    if kind == "half":
        return window(ref, row, rows, here.core * half, half)
    if kind == "columns":
        share = half // here.xs
        return window(ref, row, rows, here.core * half + x_at * share, share)
    share = rows // here.xs
    return window(ref, row + x_at * share, share, here.core * half, half)


def half_of(here, ref, shape, block):
    rows, cols = shape
    half = cols // here.cores
    return window(ref, block * rows, rows, here.core * half, half)


def gather_task(place, jobs):
    kinds = [fits(place, kind, value.shape) for kind, value in jobs]
    arrays = [value for _, value in jobs]
    shapes = [value.shape for value in arrays]
    others = place.shards - 1
    copies = sum(
        others
        + (others * (place.xs - 1) if kind in ("columns", "rows") else 0)
        + (others * (place.cores - 1) if kind != "whole" else 0)
        for kind in kinds
    )

    def run(here, copies, sources, targets, scratch):
        (own_sems,) = scratch

        def fetched(job, z_back, y_back, x_back=0):
            kind, shape = kinds[job], shapes[job]
            x_at = lax.rem(here.x - x_back + here.xs, here.xs)
            target = part_of(here, kind, targets[job], shape, here.block(z_back, y_back), x_at)
            if z_back == 0 and y_back == 0:
                return part_of(here, kind, sources[job], shape, 0, x_at), target
            return target, target

        own = []
        along_z, along_y, along_x, along_core = {}, {}, {}, {}
        for step in range(here.zs + 3):
            for job, kind in enumerate(kinds):
                z_back = step
                if z_back < here.zs:
                    if z_back > 0:
                        along_z[job, z_back - 1].wait_recv()
                    if z_back < here.zs - 1:
                        along_z[job, z_back] = copies.send(
                            *fetched(job, z_back, 0), here.device(z=1)
                        )
                    if here.ys > 1:
                        along_y[job, z_back, 0] = copies.send(
                            *fetched(job, z_back, 0), here.device(y=1)
                        )
                if step == 0:
                    rows = shapes[job][0]
                    row = pl.multiple_of(here.block(0, 0) * rows, 16)
                    copy = pltpu.make_async_copy(
                        sources[job], targets[job].at[pl.ds(row, rows), :], own_sems.at[job]
                    )
                    copy.start()
                    own.append(copy)
                z_back = step - 1
                if 0 <= z_back < here.zs:
                    for y_back in range(1, here.ys):
                        along_y[job, z_back, y_back - 1].wait_recv()
                        if y_back < here.ys - 1:
                            along_y[job, z_back, y_back] = copies.send(
                                *fetched(job, z_back, y_back), here.device(y=1)
                            )
                    if kind in ("columns", "rows") and here.xs > 1:
                        for y_back in range(0 if z_back else 1, here.ys):
                            along_x[job, z_back, y_back, 0] = copies.send(
                                *fetched(job, z_back, y_back), here.device(x=1)
                            )
                z_back = step - 2
                if 0 <= z_back < here.zs and kind != "whole":
                    for y_back in range(0 if z_back else 1, here.ys):
                        if kind != "half":
                            for x_back in range(1, here.xs):
                                along_x[job, z_back, y_back, x_back - 1].wait_recv()
                                if x_back < here.xs - 1:
                                    along_x[job, z_back, y_back, x_back] = copies.send(
                                        *fetched(job, z_back, y_back, x_back), here.device(x=1)
                                    )
                        half = half_of(here, targets[job], shapes[job], here.block(z_back, y_back))
                        along_core[job, z_back, y_back] = copies.send(
                            half, half, here.device(core=1)
                        )
                z_back = step - 3
                if 0 <= z_back < here.zs and kind != "whole":
                    for y_back in range(0 if z_back else 1, here.ys):
                        along_core[job, z_back, y_back].wait_recv()
            yield
        for copy in own:
            copy.wait()

    return Task(
        run,
        [(value, VMEM_BLOCK) for value in arrays],
        [
            (jax.ShapeDtypeStruct((place.shards * a.shape[0], a.shape[1]), a.dtype), ANY_BLOCK)
            for a in arrays
        ],
        [pltpu.SemaphoreType.DMA((len(jobs),))],
        copies,
    )


def share_of(place, kind, rows, cols):
    if kind == "columns":
        return rows, cols // place.xs
    if kind == "rows":
        return rows // place.xs, cols
    return rows, cols


def x_window(kind, ref, shape, x_at):
    rows, cols = shape
    lead = (slice(None),) * (len(ref.shape) - 2)
    if kind == "columns":
        return ref.at[lead + (slice(None), pl.ds(pl.multiple_of(x_at * cols, 128), cols))]
    return ref.at[lead + (pl.ds(pl.multiple_of(x_at * rows, 16), rows), slice(None))]


def reduce_task(place, jobs):
    zs, ys, xs = place.zs, place.ys, place.xs
    arrays = [value.reshape(place.shards, -1, value.shape[1]) for _, _, value in jobs]
    kinds = [fits(place, kind, value.shape[1:]) for (kind, _, _), value in zip(jobs, arrays)]
    behind = [late for _, late, _ in jobs]
    halves = [(value.shape[1], value.shape[2] // place.cores) for value in arrays]
    shares = [share_of(place, kind, *half) for kind, half in zip(kinds, halves)]
    count = len(jobs)
    own, got, x_got, y_got, z_got, x_sum, done = ([] for _ in range(7))
    copies = 0
    for kind, half, share in zip(kinds, halves, shares):
        split = kind != "half"
        tiny = (16, 128)
        own.append(pltpu.VMEM((2, ys) + half, BF16))
        got.append(pltpu.VMEM((zs, ys) + half, BF16))
        x_got.append(pltpu.VMEM((zs, xs - 1, ys) + share if split else tiny, BF16))
        y_got.append(pltpu.VMEM((zs, ys - 1) + share, BF16))
        z_got.append(pltpu.VMEM((zs - 1,) + share, BF16))
        x_sum.append(pltpu.VMEM(tiny if split else (xs,) + share, BF16))
        done.append(pltpu.VMEM((2,) + half, BF16))
        copies += zs + (zs * (xs - 1) if split else 0) + zs * (ys - 1) + (zs - 1) + (xs - 1) + 1

    def run(here, copies, grads, outs, scratch):
        own, got, x_got, y_got, z_got, x_sum, done = (
            scratch[at * count : (at + 1) * count] for at in range(7)
        )
        own_sems = scratch[-1]

        def target_z(t):
            return lax.rem(here.z + 2 * zs - 1 - t, zs)

        def half_at(job, t, core):
            half = halves[job][1]
            return grads[job].at[
                pl.ds(target_z(t) * ys, ys), :, pl.ds(pl.multiple_of(core * half, 128), half)
            ]

        def load(job, t):
            copy = pltpu.make_async_copy(
                half_at(job, t, here.core), own[job].at[t % 2], own_sems.at[job, t % 2]
            )
            copy.start()
            return copy

        loads, by_core = {}, {}
        for wave in range(zs + max(behind)):
            for job in range(count):
                t = wave - behind[job]
                if 0 <= t < zs:
                    by_core[job, t] = copies.send(
                        half_at(job, t, lax.rem(here.core + 1, here.cores)),
                        got[job].at[t],
                        here.device(core=1),
                    )
                    if t < 2:
                        loads[job, t] = load(job, t)
        yield
        by_x, by_y, by_z = {}, {}, {}

        def base(job, t):
            return got[job].at[t] if kinds[job] == "half" else x_got[job].at[t, 0]

        def send_y(job, t):
            for turn in range(1, ys):
                by_y[job, t, turn] = copies.send(
                    base(job, t).at[lax.rem(here.y + turn, ys)],
                    y_got[job].at[t, turn - 1],
                    here.device(y=turn),
                )

        for step in range(zs + 4 + max(behind)):
            for job, kind in enumerate(kinds):
                rows, cols = shares[job]
                local = step - behind[job]
                t = local
                if 0 <= t < zs:
                    loads[job, t].wait()
                    by_core[job, t].wait_recv()
                    for y in range(ys):
                        mine, sums = own[job].at[t % 2, y], got[job].at[t, y]

                        def both(at, mine=mine, sums=sums):
                            sums[at] = (mine[at].astype(F32) + sums[at].astype(F32)).astype(BF16)

                        by_rows(halves[job][0], both)
                    if t + 2 < zs:
                        loads[job, t + 2] = load(job, t + 2)
                    if kind == "half":
                        send_y(job, t)
                    else:
                        for turn in range(1, xs):
                            x_at = lax.rem(here.x + turn, xs)
                            by_x[job, t, turn] = copies.send(
                                x_window(kind, got[job].at[t], shares[job], x_at),
                                x_got[job].at[t, turn - 1],
                                here.device(x=turn),
                            )
                t = local - 1
                if 0 <= t < zs and kind != "half":
                    for turn in range(1, xs):
                        by_x[job, t, turn].wait_recv()
                    for y in range(ys):
                        mine = x_window(kind, got[job].at[t, y], shares[job], here.x)
                        parts = [x_got[job].at[t, turn, y] for turn in range(xs - 1)]

                        def all_x(at, mine=mine, parts=parts):
                            total = mine[at].astype(F32)
                            for part in parts:
                                total += part[at].astype(F32)
                            parts[0][at] = total.astype(BF16)

                        by_rows(rows, all_x)
                    send_y(job, t)
                t = local - 2
                if 0 <= t < zs:
                    for turn in range(1, ys):
                        by_y[job, t, turn].wait_recv()
                    parts = [y_got[job].at[t, turn] for turn in range(ys - 1)]
                    target = parts[0]
                    if t > 0:
                        by_z[job, t - 1].wait_recv()
                        parts.append(z_got[job].at[t - 1])
                    if t == zs - 1:
                        target = (
                            x_sum[job].at[here.x]
                            if kind == "half"
                            else x_window(kind, done[job].at[0], shares[job], here.x)
                        )
                    mine = base(job, t).at[here.y]

                    def all_y(at, mine=mine, parts=parts, target=target):
                        total = mine[at].astype(F32)
                        for part in parts:
                            total += part[at].astype(F32)
                        target[at] = total.astype(BF16)

                    by_rows(rows, all_y)
                    if t < zs - 1:
                        by_z[job, t] = copies.send(target, z_got[job].at[t], here.device(z=1))
                    else:
                        for turn in range(1, xs):
                            by_x[job, "done", turn] = copies.send(
                                target, target, here.device(x=turn)
                            )
                if local == zs + 2:
                    for turn in range(1, xs):
                        by_x[job, "done", turn].wait_recv()
                    if kind == "half":
                        sums, target = x_sum[job], done[job].at[0]

                        def across(at, sums=sums, target=target):
                            total = sums[0, at].astype(F32)
                            for x_at in range(1, xs):
                                total += sums[x_at, at].astype(F32)
                            target[at] = total.astype(BF16)

                        by_rows(rows, across)
                    by_core[job, "done"] = copies.send(
                        done[job].at[0], done[job].at[1], here.device(core=1)
                    )
                if local == zs + 3:
                    by_core[job, "done"].wait_recv()
                    half_rows, half = halves[job]
                    for side in range(2):
                        column = lax.rem(here.core + side, 2) * half
                        place_at = outs[job].at[:, pl.ds(pl.multiple_of(column, 128), half)]

                        def write(at, place_at=place_at, source=done[job].at[side]):
                            place_at[at] = source[at].astype(F32)

                        by_rows(half_rows, write)
            yield

    return Task(
        run,
        [(value, ANY_BLOCK) for value in arrays],
        [(jax.ShapeDtypeStruct(value.shape[1:], F32), VMEM_BLOCK) for value in arrays],
        own
        + got
        + x_got
        + y_got
        + z_got
        + x_sum
        + done
        + [pltpu.SemaphoreType.DMA((count, 2))],
        copies,
    )


def reduce_vectors_task(place, vectors):
    shape = vectors.shape[1:]

    def run(here, copies, ins, outs, scratch):
        (vec_ref,), (out_ref,), (got, sums) = ins, outs, scratch
        arriving = []
        for step in range(1, here.shards):
            to = lax.rem(here.s + step, here.shards)
            device = {"replica": here.r, "shard": to}
            arriving.append(copies.send(vec_ref.at[to], got.at[step - 1], device))
        yield
        yield
        yield
        for copy in arriving:
            copy.wait_recv()
        total = vec_ref[here.s]
        for at in range(here.shards - 1):
            total += got[at]
        sums[here.r] = total
        arriving = []
        for step in range(1, here.replicas):
            device = {"replica": lax.rem(here.r + step, here.replicas), "shard": here.s}
            arriving.append(copies.send(sums.at[here.r], sums.at[here.r], device))
        yield
        yield
        for copy in arriving:
            copy.wait_recv()
        total = sums[0]
        for at in range(1, here.replicas):
            total += sums[at]
        out_ref[...] = total

    return Task(
        run,
        [(vectors, VMEM_BLOCK)],
        [(jax.ShapeDtypeStruct(shape, F32), VMEM_BLOCK)],
        [
            pltpu.VMEM((place.shards - 1,) + shape, F32),
            pltpu.VMEM((place.replicas,) + shape, F32),
        ],
        place.shards + place.replicas - 2,
    )


def pack_lanes(values, lead):
    size = values.shape[-1]
    lanes = 128 * -(-size // (16 * 128))
    values = jnp.pad(values, [(0, 0)] * len(lead) + [(0, 16 * lanes - size)])
    return values.reshape(lead + (16, lanes))


def unpack_vectors(flat, layers, sizes):
    flat = flat[..., : layers * sum(sizes)]
    flat = flat.reshape(flat.shape[:-1] + (layers, -1))
    out, start = [], 0
    for size in sizes:
        out.append(flat[..., start : start + size])
        start += size
    return out


def per_device(
    tokens,
    gain_one,
    shift_one,
    query_key_value_weight,
    b_query,
    b_value,
    output_weight,
    output_proj_bias,
    gain_two,
    shift_two,
    up_weight,
    up_bias,
    down_weight,
    down_bias,
    cotangent,
):
    place = Place(lax.axis_size("replica"), lax.axis_size("shard")).locate()
    held, _, width = tokens.shape
    layers = gain_one.shape[0]
    last = layers - 1
    mix = place.mix_columns(query_key_value_weight)
    vectors = (
        gain_one,
        shift_one,
        b_query,
        b_value,
        output_proj_bias,
        gain_two,
        shift_two,
        up_bias,
        down_bias,
    )
    sizes = [vector.shape[1] for vector in vectors]
    packed = pack_lanes(jnp.concatenate(vectors, -1).reshape(-1), ())
    current = place.to_sequences(tokens).astype(F32)

    ((whole_vectors, first_mix),) = fuse(
        place, "gather_first", 0, [gather_task(place, [("whole", packed), ("half", mix[0])])], ()
    )
    flat = whole_vectors.reshape(place.shards, -1)
    g1, s1, bq, bv, bo, g2, s2, bu, bd = (
        jnp.swapaxes(piece, 0, 1).reshape(layers, -1).astype(F32)
        for piece in unpack_vectors(flat, layers, sizes)
    )
    mix_bias = place.mix_columns(jnp.concatenate([bq, jnp.zeros_like(bq), bv], -1))
    mixes, outs = [first_mix], []
    ups, downs = [], []

    saved = []
    for n in range(layers):
        normed = norm_rows(current, g1[n], s1[n]).astype(BF16)
        mixed = (dot(normed, mixes[n], ((1,), (0,))) + mix_bias[n]).astype(BF16)
        jobs = [("columns", up_weight[n]), ("rows" if n < last else "half", down_weight[n])]
        if n == 0:
            jobs.append(("half", output_weight[0]))
        if n < last:
            jobs += [("half", mix[n + 1]), ("half", output_weight[n + 1])]
        (seq, attended), gathered = fuse(
            place,
            f"attend_{n}",
            1 + n,
            [attend_task(place, mixed), gather_task(place, jobs)],
            (0, 1, 1, 0) + (0, 1) * place.replicas,
        )
        ups.append(gathered.pop(0))
        downs.append(gathered.pop(0))
        if n == 0:
            outs.append(gathered.pop(0))
        if n < last:
            mixes.append(gathered.pop(0))
            outs.append(gathered.pop(0))
        x_mid = current + (dot(attended, outs[n], ((1,), (0,))) + bo[n])
        moved = norm_rows(x_mid, g2[n], s2[n]).astype(BF16)
        pre = dot(moved, ups[n], ((1,), (0,))) + bu[n]
        act = jax.nn.gelu(pre, approximate=True).astype(BF16)
        saved.append((current, normed, seq, attended, x_mid, moved, pre, act))
        current = x_mid + dot(act, downs[n], ((1,), (0,))) + bd[n]
    output = place.from_sequences(current.astype(BF16), held)

    grad_now = place.to_sequences(cotangent).astype(F32)
    summed = [{} for _ in range(layers)]
    vector_grads = [None] * layers
    waiting = []
    for n in reversed(range(layers)):
        current, normed, seq, attended, x_mid, moved, pre, act = saved[n]
        d_ffn = grad_now.astype(BF16)
        grad_down = dot(act, d_ffn, ((0,), (0,))).astype(BF16)
        grad_b_down = jnp.sum(d_ffn.astype(F32), 0)
        d_act = dot(d_ffn, downs[n], ((1,), (1,)))
        gelu_back = jax.vjp(lambda inner: jax.nn.gelu(inner, approximate=True), pre)[1]
        d_pre = gelu_back(d_act)[0].astype(BF16)
        grad_up = dot(moved, d_pre, ((0,), (0,))).astype(BF16)
        grad_b_up = jnp.sum(d_pre.astype(F32), 0)
        d_moved = dot(d_pre, ups[n], ((1,), (1,)))
        norm_back = jax.vjp(norm_rows, x_mid, g2[n], s2[n])[1]
        d_from_norm, grad_gain_two, grad_shift_two = norm_back(d_moved)
        grad_mid = grad_now + d_from_norm
        d_branch = grad_mid.astype(BF16)
        grad_out = dot(attended, d_branch, ((0,), (0,))).astype(BF16)
        grad_b_out = jnp.sum(d_branch.astype(F32), 0)
        d_att = dot(d_branch, outs[n], ((1,), (1,))).astype(BF16)
        waiting += [("up", n, "columns", 0, grad_up), ("down", n, "half", 1, grad_down)]
        (d_mixed,), sums = fuse(
            place,
            f"attend_back_{n}",
            1 + layers + n,
            [
                attend_back_task(place, seq, d_att),
                reduce_task(place, [job[2:] for job in waiting]),
            ],
            (0, 1, 1, 0) + (0, 1) * place.replicas,
        )
        for job, value in zip(waiting, sums):
            summed[job[1]][job[0]] = value
        grad_mix = dot(normed, d_mixed, ((0,), (0,))).astype(BF16)
        waiting = [("mix", n, "half", 0, grad_mix), ("out", n, "half", 0, grad_out)]
        grad_b_mix = place.unmix_columns(jnp.sum(d_mixed.astype(F32), 0))
        d_normed = dot(d_mixed, mixes[n], ((1,), (1,)))
        first_back = jax.vjp(norm_rows, current, g1[n], s1[n])[1]
        d_from_first, grad_gain_one, grad_shift_one = first_back(d_normed)
        grad_now = grad_mid + d_from_first
        vector_grads[n] = (
            grad_gain_one,
            grad_shift_one,
            grad_b_mix[:width],
            grad_b_mix[2 * width :],
            grad_b_out,
            grad_gain_two,
            grad_shift_two,
            grad_b_up,
            grad_b_down,
        )
    grad_tokens = place.from_sequences(grad_now.astype(BF16), held).astype(F32)
    rows = [v.reshape(place.shards, -1) for vectors in vector_grads for v in vectors]
    packed = pack_lanes(jnp.concatenate(rows, 1), (place.shards,))
    sums, (vector_sums,) = fuse(
        place,
        "reduce_last",
        1 + 2 * layers,
        [
            reduce_task(place, [job[2:] for job in waiting]),
            reduce_vectors_task(place, packed),
        ],
        (0, 1) * 8,
    )
    for job, value in zip(waiting, sums):
        summed[job[1]][job[0]] = value
    weight_grads = {
        name: jnp.stack([summed[n][name] for n in range(layers)])
        for name in ("mix", "out", "up", "down")
    }
    own = unpack_vectors(vector_sums.reshape(-1), layers, sizes)
    (
        grad_gain_one,
        grad_shift_one,
        grad_b_query,
        grad_b_value,
        grad_b_out,
        grad_gain_two,
        grad_shift_two,
        grad_b_up,
        grad_b_down,
    ) = own
    return (
        output,
        grad_tokens,
        grad_gain_one,
        grad_shift_one,
        place.unmix_columns(weight_grads["mix"]),
        grad_b_query,
        grad_b_value,
        weight_grads["out"],
        grad_b_out,
        grad_gain_two,
        grad_shift_two,
        weight_grads["up"],
        grad_b_up,
        weight_grads["down"],
        grad_b_down,
    )


def solution(mesh):
    vector, matrix = P(None, "shard"), P(None, "shard", None)
    rows = P("replica", "shard", None)
    in_specs = (
        rows,
        vector,
        vector,
        matrix,
        vector,
        vector,
        matrix,
        vector,
        vector,
        vector,
        matrix,
        vector,
        matrix,
        vector,
        rows,
    )
    out_specs = (
        rows,
        rows,
        vector,
        vector,
        matrix,
        vector,
        vector,
        matrix,
        vector,
        vector,
        vector,
        matrix,
        vector,
        matrix,
        vector,
    )
    return jax.shard_map(
        per_device, mesh=mesh, in_specs=in_specs, out_specs=out_specs, check_vma=False
    )
```

```python
import functools

import jax
import jax.numpy as jnp
from jax import lax
from jax.experimental import pallas as pl
from jax.experimental.pallas import tpu as pltpu
from jax.sharding import PartitionSpec as P

HEADS = 12
HEAD_DIM = 64
EPSILON = 1e-05
MASKED = -1e30
F32 = jnp.float32
BF16 = jnp.bfloat16
BOTH = ("replica", "shard")
MESH = pl.DeviceIdType.MESH
VMEM_BLOCK = pl.BlockSpec(memory_space=pltpu.VMEM)
ANY_BLOCK = pl.BlockSpec(memory_space=pl.ANY)


def dot(a, b, contract):
    return lax.dot_general(a, b, (contract, ((), ())), preferred_element_type=F32)


def norm_rows(values, gain, shift):
    centre = values - jnp.mean(values, -1, keepdims=True)
    spread = jnp.mean(centre * centre, -1, keepdims=True)
    return centre * lax.rsqrt(spread + EPSILON) * gain + shift


def norm_rows_back(values, gain, grad):
    centre = values - jnp.mean(values, -1, keepdims=True)
    scale = lax.rsqrt(jnp.mean(centre * centre, -1, keepdims=True) + EPSILON)
    normal = centre * scale
    inner = grad * gain
    along = jnp.mean(inner * normal, -1, keepdims=True)
    d_values = scale * (inner - jnp.mean(inner, -1, keepdims=True) - normal * along)
    return d_values, jnp.sum(grad * normal, 0, keepdims=True), jnp.sum(grad, 0, keepdims=True)


class Place:
    def __init__(self, replicas, shards):
        self.replicas, self.shards = replicas, shards
        self.cores = 2
        self.xs = replicas // self.cores
        self.zs = 4
        self.ys = shards // self.zs
        assert self.xs * self.cores == replicas and self.zs * self.ys == shards
        self.heads = -(-HEADS // replicas)
        self.padded = self.heads * replicas
        self.span = 3 * self.heads * HEAD_DIM
        self.columns = 128 * -(-self.span // 128)

    def locate(self):
        self.r, self.s = lax.axis_index("replica"), lax.axis_index("shard")
        self.x, self.core = self.r // self.cores, lax.rem(self.r, self.cores)
        self.z, self.y = self.s // self.ys, lax.rem(self.s, self.ys)
        return self

    def device(self, x=0, core=0, z=0, y=0):
        to_x = lax.rem(self.x + x + self.xs, self.xs)
        to_core = lax.rem(self.core + core, self.cores)
        to_z = lax.rem(self.z + z + self.zs, self.zs)
        to_y = lax.rem(self.y + y + self.ys, self.ys)
        return {"replica": to_x * self.cores + to_core, "shard": to_z * self.ys + to_y}

    def block(self, z_back, y_back):
        from_z = lax.rem(self.z - z_back + self.zs, self.zs)
        from_y = lax.rem(self.y - y_back + self.ys, self.ys)
        return from_z * self.ys + from_y

    def turn_pairs(self, turn, held):
        pairs = []
        for r in range(self.replicas):
            for s in range(self.shards):
                target = (s // held) * self.shards + held * r + (s + turn) % held
                pairs.append((r * self.shards + s, target))
        return pairs

    def to_sequences(self, blocks):
        held = blocks.shape[0]
        assert held * self.replicas == self.shards
        got = []
        for turn in range(held):
            block = lax.dynamic_index_in_dim(blocks, (self.s + turn) % held, 0, keepdims=False)
            got.append(lax.ppermute(block, BOTH, self.turn_pairs(turn, held)))
        stacked = jnp.stack(got)
        ordered = [
            lax.dynamic_index_in_dim(stacked, (self.s - u) % held, 0, keepdims=False)
            for u in range(held)
        ]
        return jnp.concatenate(ordered, 0)

    def from_sequences(self, values, held):
        blocks = values.reshape(held, -1, values.shape[-1])
        got = []
        for turn in range(held):
            pairs = [(b, a) for a, b in self.turn_pairs(turn, held)]
            block = lax.dynamic_index_in_dim(blocks, (self.s - turn) % held, 0, keepdims=False)
            got.append(lax.ppermute(block, BOTH, pairs))
        stacked = jnp.stack(got)
        return jnp.stack(
            [
                lax.dynamic_index_in_dim(stacked, (i - self.s) % held, 0, keepdims=False)
                for i in range(held)
            ]
        )

    def mix_columns(self, weight):
        lead = weight.shape[:-1]
        parts = weight.reshape(lead + (3, HEADS, HEAD_DIM))
        extra = [(0, 0)] * len(lead) + [(0, 0), (0, self.padded - HEADS), (0, 0)]
        parts = jnp.pad(parts, extra)
        parts = parts.reshape(lead + (3, self.replicas, self.heads * HEAD_DIM))
        parts = jnp.swapaxes(parts, -3, -2).reshape(lead + (self.replicas, self.span))
        parts = jnp.pad(parts, [(0, 0)] * (len(lead) + 1) + [(0, self.columns - self.span)])
        return parts.reshape(lead + (-1,))


class Copies:
    def __init__(self, send_sems, recv_sems):
        self.send_sems, self.recv_sems, self.started = send_sems, recv_sems, []

    def send(self, source, target, device):
        at = len(self.started)
        copy = pltpu.make_async_remote_copy(
            src_ref=source,
            dst_ref=target,
            send_sem=self.send_sems.at[at],
            recv_sem=self.recv_sems.at[at],
            device_id=device,
            device_id_type=MESH,
        )
        copy.start()
        self.started.append(copy)
        return copy

    def finish(self):
        for copy in self.started:
            copy.wait_send()


class Task:
    def __init__(self, run, inputs, outputs, scratch, copies):
        self.run, self.inputs, self.outputs = run, inputs, outputs
        self.scratch, self.copies = scratch, copies


def fuse(place, name, collective_id, tasks, order):
    sizes = (place.replicas, place.shards)
    count = sum(task.copies for task in tasks)

    def kernel(*refs):
        here = Place(*sizes).locate()
        refs = list(refs)

        def take(number):
            taken = refs[:number]
            del refs[:number]
            return taken

        ins = [take(len(task.inputs)) for task in tasks]
        outs = [take(len(task.outputs)) for task in tasks]
        own = [take(len(task.scratch)) for task in tasks]
        copies = Copies(*refs)
        barrier = pltpu.get_barrier_semaphore()
        for step in range(1, here.shards):
            peer = {"replica": here.r, "shard": lax.rem(here.s + step, here.shards)}
            pl.semaphore_signal(barrier, 1, device_id=peer, device_id_type=MESH)
        for step in range(1, here.replicas):
            peer = {"replica": lax.rem(here.r + step, here.replicas), "shard": here.s}
            pl.semaphore_signal(barrier, 1, device_id=peer, device_id_type=MESH)
        pl.semaphore_wait(barrier, here.shards + here.replicas - 2)
        streams = [
            task.run(here, copies, *group) for task, *group in zip(tasks, ins, outs, own)
        ]
        for at in order:
            next(streams[at], None)
        for stream in streams:
            for _ in stream:
                pass
        copies.finish()

    results = pl.pallas_call(
        kernel,
        out_shape=[shape for task in tasks for shape, _ in task.outputs],
        in_specs=[spec for task in tasks for _, spec in task.inputs],
        out_specs=[spec for task in tasks for _, spec in task.outputs],
        scratch_shapes=[shape for task in tasks for shape in task.scratch]
        + [pltpu.SemaphoreType.DMA((count,)), pltpu.SemaphoreType.DMA((count,))],
        compiler_params=pltpu.CompilerParams(
            collective_id=collective_id,
            has_side_effects=True,
            vmem_limit_bytes=60 * 1024 * 1024,
        ),
        name=name,
    )(*[value for task in tasks for value, _ in task.inputs])
    split, start = [], 0
    for task in tasks:
        split.append(list(results[start : start + len(task.outputs)]))
        start += len(task.outputs)
    return split


def by_rows(rows, body):
    @pl.loop(0, rows // 16)
    def _(at):
        body(pl.ds(pl.multiple_of(at * 16, 16), 16))


def block_probs(q_ref, k_ref, head, first, rows):
    count = first + rows
    query = q_ref[head, first:count, :]
    keys = k_ref[head, 0:count, :]
    scores = dot(query, keys, ((1,), (1,))) * (HEAD_DIM**-0.5)
    row = lax.broadcasted_iota(jnp.int32, (rows, count), 0) + first
    col = lax.broadcasted_iota(jnp.int32, (rows, count), 1)
    scores = jnp.where(row >= col, scores, MASKED)
    expo = jnp.exp(scores - jnp.max(scores, -1, keepdims=True))
    return expo / jnp.sum(expo, -1, keepdims=True), query, keys


def split_heads(source, targets):
    for place, target in enumerate(targets):
        heads = target.shape[0]
        for head in range(heads):
            start = (place * heads + head) * HEAD_DIM
            target[head] = source[:, start : start + HEAD_DIM]


class Blocks:
    def __init__(self, here, ready, land, send_sems, recv_sems):
        self.here, self.ready, self.land = here, ready, land
        self.send_sems, self.recv_sems = send_sems, recv_sems

    def copy(self, at, source):
        here = self.here
        return pltpu.make_async_remote_copy(
            src_ref=self.ready.at[at],
            dst_ref=self.land(source),
            send_sem=self.send_sems.at[at],
            recv_sem=self.recv_sems.at[source],
            device_id={"replica": at, "shard": here.s},
            device_id_type=MESH,
        )

    def send(self, at):
        here = self.here

        @pl.when(here.r != at)
        def _():
            self.copy(at, here.r).start()

        @pl.when(here.r == at)
        def _():
            self.land(at)[...] = self.ready[at]

    def finish(self):
        for at in range(self.here.replicas):

            @pl.when(self.here.r != at)
            def _(at=at):
                self.copy(at, at).wait_recv()
                self.copy(at, at).wait_send()


def attend_task(place, mixed):
    rows, replicas, heads, columns = mixed.shape[0], place.replicas, place.heads, place.columns
    length, wide = rows * replicas, heads * HEAD_DIM

    def run(here, copies, ins, outs, scratch):
        (mixed_ref,), (seq_ref, out_ref) = ins, outs
        q_ref, k_ref, v_ref, o_ref, ready, landed, send_sems, recv_sems = scratch
        mine = pl.ds(pl.multiple_of(here.r * rows, 16), rows)
        arriving = []
        for step in range(1, replicas):
            to = lax.rem(here.r + step, replicas)
            source = mixed_ref.at[:, pl.ds(pl.multiple_of(to * columns, 128), columns)]
            device = {"replica": to, "shard": here.s}
            arriving.append(copies.send(source, seq_ref.at[mine, :], device))
        seq_ref[mine, :] = mixed_ref[:, pl.ds(pl.multiple_of(here.r * columns, 128), columns)]
        yield
        for copy in arriving:
            copy.wait_recv()
        split_heads(seq_ref, (q_ref, k_ref, v_ref))
        blocks = Blocks(here, ready, lambda at: landed.at[at], send_sems, recv_sems)
        yield
        for at in range(replicas):
            first = at * rows

            @pl.loop(0, heads)
            def _(head, first=first):
                probs, _, _ = block_probs(q_ref, k_ref, head, first, rows)
                keys = v_ref[head, 0 : first + rows, :]
                o_ref[head] = dot(probs.astype(BF16), keys, ((1,), (0,))).astype(BF16)

            for head in range(heads):
                ready[at, :, head * HEAD_DIM : (head + 1) * HEAD_DIM] = o_ref[head]
            blocks.send(at)
            yield
        blocks.finish()
        width = out_ref.shape[1]
        for at in range(replicas):
            start = at * wide
            size = min(wide, width - start)
            if size > 0:
                out_ref[:, start : start + size] = landed[at, :, :size]

    part = pltpu.VMEM((heads, length, HEAD_DIM), BF16)
    return Task(
        run,
        [(mixed, VMEM_BLOCK)],
        [
            (jax.ShapeDtypeStruct((length, columns), BF16), VMEM_BLOCK),
            (jax.ShapeDtypeStruct((rows, HEADS * HEAD_DIM), BF16), VMEM_BLOCK),
        ],
        [part] * 3
        + [pltpu.VMEM((heads, rows, HEAD_DIM), BF16)]
        + [pltpu.VMEM((replicas, rows, wide), BF16)] * 2
        + [pltpu.SemaphoreType.DMA((replicas,))] * 2,
        replicas - 1,
    )


def attend_back_task(place, seq, d_attended):
    rows, width = d_attended.shape
    replicas, heads, columns = place.replicas, place.heads, place.columns
    length, wide = rows * replicas, heads * HEAD_DIM

    def run(here, copies, ins, outs, scratch):
        (seq_ref, d_ref), (out_ref,) = ins, outs
        q_ref, k_ref, v_ref, do_ref, dq_ref, dk_ref, dv_ref = scratch[:7]
        d_ready, d_landed, ready, send_sems, recv_sems = scratch[7:]
        for at in range(replicas):
            start = at * wide
            size = max(0, min(wide, width - start))
            if size > 0:
                d_ready[at, :, :size] = d_ref[:, start : start + size]
            if size < wide:
                d_ready[at, :, size:] = jnp.zeros((rows, wide - size), BF16)
        arriving = []
        for step in range(1, replicas):
            to = lax.rem(here.r + step, replicas)
            device = {"replica": to, "shard": here.s}
            arriving.append(copies.send(d_ready.at[to], d_landed.at[here.r], device))
        d_landed[here.r] = d_ready[here.r]
        yield
        split_heads(seq_ref, (q_ref, k_ref, v_ref))
        dk_ref[...] = jnp.zeros((heads, length, HEAD_DIM), F32)
        dv_ref[...] = jnp.zeros((heads, length, HEAD_DIM), F32)
        for copy in arriving:
            copy.wait_recv()
        for at in range(replicas):
            for head in range(heads):
                do_ref[head, at * rows : (at + 1) * rows, :] = d_landed[
                    at, :, head * HEAD_DIM : (head + 1) * HEAD_DIM
                ]

        def land(source):
            return out_ref.at[:, pl.ds(pl.multiple_of(source * columns, 128), columns)]

        blocks = Blocks(here, ready, land, send_sems, recv_sems)
        yield
        for at in reversed(range(replicas)):
            first = at * rows
            count = first + rows

            @pl.loop(0, heads)
            def _(head, first=first, count=count):
                probs, query, keys = block_probs(q_ref, k_ref, head, first, rows)
                d_out = do_ref[head, first:count, :]
                d_probs = dot(d_out, v_ref[head, 0:count, :], ((1,), (1,)))
                row_dot = jnp.sum(d_probs * probs, -1, keepdims=True)
                d_scores = (probs * (d_probs - row_dot) * (HEAD_DIM**-0.5)).astype(BF16)
                dq_ref[head] = dot(d_scores, keys, ((1,), (0,))).astype(BF16)
                dk_ref[head, 0:count, :] += dot(d_scores, query, ((0,), (0,)))
                dv_ref[head, 0:count, :] += dot(probs.astype(BF16), d_out, ((0,), (0,)))

            for head in range(heads):
                pieces = (
                    dq_ref[head],
                    dk_ref[head, first:count, :].astype(BF16),
                    dv_ref[head, first:count, :].astype(BF16),
                )
                for part, piece in enumerate(pieces):
                    start = (part * heads + head) * HEAD_DIM
                    ready[at, :, start : start + HEAD_DIM] = piece
            if place.span < columns:
                ready[at, :, place.span :] = jnp.zeros((rows, columns - place.span), BF16)
            blocks.send(at)
            yield
        blocks.finish()

    part = pltpu.VMEM((heads, length, HEAD_DIM), BF16)
    sums = pltpu.VMEM((heads, length, HEAD_DIM), F32)
    return Task(
        run,
        [(seq, VMEM_BLOCK), (d_attended, VMEM_BLOCK)],
        [(jax.ShapeDtypeStruct((rows, replicas * columns), BF16), VMEM_BLOCK)],
        [part] * 4
        + [pltpu.VMEM((heads, rows, HEAD_DIM), BF16), sums, sums]
        + [pltpu.VMEM((replicas, rows, wide), BF16)] * 2
        + [pltpu.VMEM((replicas, rows, columns), BF16)]
        + [pltpu.SemaphoreType.DMA((replicas,))] * 2,
        replicas - 1,
    )


def fits(place, kind, shape):
    rows, half = shape[0], shape[1] // place.cores
    if kind == "columns" and half % (128 * place.xs):
        return "half"
    if kind == "rows" and rows % (16 * place.xs):
        return "half"
    return kind


def window(ref, row, rows, col, cols):
    row = row if isinstance(row, int) else pl.multiple_of(row, 16)
    col = col if isinstance(col, int) else pl.multiple_of(col, 128)
    return ref.at[pl.ds(row, rows), pl.ds(col, cols)]


def part_of(here, kind, ref, shape, block, x_at):
    rows, cols = shape
    row = block * rows
    if kind == "whole":
        return window(ref, row, rows, 0, cols)
    half = cols // here.cores
    if kind == "half":
        return window(ref, row, rows, here.core * half, half)
    if kind == "columns":
        share = half // here.xs
        return window(ref, row, rows, here.core * half + x_at * share, share)
    share = rows // here.xs
    return window(ref, row + x_at * share, share, here.core * half, half)


def half_of(here, ref, shape, block):
    rows, cols = shape
    half = cols // here.cores
    return window(ref, block * rows, rows, here.core * half, half)


def gather_task(place, jobs):
    kinds = [fits(place, kind, value.shape) for kind, value in jobs]
    arrays = [value for _, value in jobs]
    shapes = [value.shape for value in arrays]
    others = place.shards - 1
    copies = sum(
        others
        + (others * (place.xs - 1) if kind in ("columns", "rows") else 0)
        + (others * (place.cores - 1) if kind != "whole" else 0)
        for kind in kinds
    )

    def run(here, copies, sources, targets, scratch):
        (own_sems,) = scratch

        def fetched(job, z_back, y_back, x_back=0):
            kind, shape = kinds[job], shapes[job]
            x_at = lax.rem(here.x - x_back + here.xs, here.xs)
            target = part_of(here, kind, targets[job], shape, here.block(z_back, y_back), x_at)
            if z_back == 0 and y_back == 0:
                return part_of(here, kind, sources[job], shape, 0, x_at), target
            return target, target

        own = []
        along_z, along_y, along_x, along_core = {}, {}, {}, {}
        for step in range(here.zs + 3):
            for job, kind in enumerate(kinds):
                z_back = step
                if z_back < here.zs:
                    if z_back > 0:
                        along_z[job, z_back - 1].wait_recv()
                    if z_back < here.zs - 1:
                        along_z[job, z_back] = copies.send(
                            *fetched(job, z_back, 0), here.device(z=1)
                        )
                    if here.ys > 1:
                        along_y[job, z_back, 0] = copies.send(
                            *fetched(job, z_back, 0), here.device(y=1)
                        )
                if step == 0:
                    rows = shapes[job][0]
                    row = pl.multiple_of(here.block(0, 0) * rows, 16)
                    copy = pltpu.make_async_copy(
                        sources[job], targets[job].at[pl.ds(row, rows), :], own_sems.at[job]
                    )
                    copy.start()
                    own.append(copy)
                z_back = step - 1
                if 0 <= z_back < here.zs:
                    for y_back in range(1, here.ys):
                        along_y[job, z_back, y_back - 1].wait_recv()
                        if y_back < here.ys - 1:
                            along_y[job, z_back, y_back] = copies.send(
                                *fetched(job, z_back, y_back), here.device(y=1)
                            )
                    if kind in ("columns", "rows") and here.xs > 1:
                        for y_back in range(0 if z_back else 1, here.ys):
                            along_x[job, z_back, y_back, 0] = copies.send(
                                *fetched(job, z_back, y_back), here.device(x=1)
                            )
                z_back = step - 2
                if 0 <= z_back < here.zs and kind != "whole":
                    for y_back in range(0 if z_back else 1, here.ys):
                        if kind != "half":
                            for x_back in range(1, here.xs):
                                along_x[job, z_back, y_back, x_back - 1].wait_recv()
                                if x_back < here.xs - 1:
                                    along_x[job, z_back, y_back, x_back] = copies.send(
                                        *fetched(job, z_back, y_back, x_back), here.device(x=1)
                                    )
                        half = half_of(here, targets[job], shapes[job], here.block(z_back, y_back))
                        along_core[job, z_back, y_back] = copies.send(
                            half, half, here.device(core=1)
                        )
                z_back = step - 3
                if 0 <= z_back < here.zs and kind != "whole":
                    for y_back in range(0 if z_back else 1, here.ys):
                        along_core[job, z_back, y_back].wait_recv()
            yield
        for copy in own:
            copy.wait()

    return Task(
        run,
        [(value, VMEM_BLOCK) for value in arrays],
        [
            (jax.ShapeDtypeStruct((place.shards * a.shape[0], a.shape[1]), a.dtype), ANY_BLOCK)
            for a in arrays
        ],
        [pltpu.SemaphoreType.DMA((len(jobs),))],
        copies,
    )


def share_of(place, kind, rows, cols):
    if kind == "columns":
        return rows, cols // place.xs
    if kind == "rows":
        return rows // place.xs, cols
    return rows, cols


def x_window(kind, ref, shape, x_at):
    rows, cols = shape
    lead = (slice(None),) * (len(ref.shape) - 2)
    if kind == "columns":
        return ref.at[lead + (slice(None), pl.ds(pl.multiple_of(x_at * cols, 128), cols))]
    return ref.at[lead + (pl.ds(pl.multiple_of(x_at * rows, 16), rows), slice(None))]


def unmix(here, halves, out, core, shape):
    rows, half = shape
    part = here.heads * HEAD_DIM
    width = out.shape[1] // 3

    def write(at):
        for r in range(here.replicas):
            side, start = divmod(r * here.columns, half)
            size = min(part, width - r * part)
            if size > 0:
                values = halves[(side + core) % 2, at, start : start + here.span].astype(F32)
                for place_at in range(3):
                    to = place_at * width + r * part
                    out[at, to : to + size] = values[:, place_at * part : place_at * part + size]

    by_rows(rows, write)


def reduce_task(place, jobs):
    zs, ys, xs = place.zs, place.ys, place.xs
    arrays = [value.reshape(place.shards, -1, value.shape[1]) for _, _, value in jobs]
    kinds = [fits(place, kind, value.shape[1:]) for (kind, _, _), value in zip(jobs, arrays)]
    behind = [0] * len(jobs)
    mixed = [natural for _, natural, _ in jobs]
    halves = [(value.shape[1], value.shape[2] // place.cores) for value in arrays]
    shares = [share_of(place, kind, *half) for kind, half in zip(kinds, halves)]
    count = len(jobs)
    own, got, x_got, y_got, z_got, x_sum, done = ([] for _ in range(7))
    copies = 0
    for kind, half, share in zip(kinds, halves, shares):
        split = kind != "half"
        tiny = (16, 128)
        own.append(pltpu.VMEM((2, ys) + half, BF16))
        got.append(pltpu.VMEM((zs, ys) + half, BF16))
        x_got.append(pltpu.VMEM((zs, xs - 1, ys) + share if split else tiny, BF16))
        y_got.append(pltpu.VMEM((zs, ys - 1) + share, BF16))
        z_got.append(pltpu.VMEM((zs - 1,) + share, BF16))
        x_sum.append(pltpu.VMEM(tiny if split else (xs,) + share, BF16))
        done.append(pltpu.VMEM((2,) + half, BF16))
        copies += zs + (zs * (xs - 1) if split else 0) + zs * (ys - 1) + (zs - 1) + (xs - 1) + 1

    def run(here, copies, grads, outs, scratch):
        own, got, x_got, y_got, z_got, x_sum, done = (
            scratch[at * count : (at + 1) * count] for at in range(7)
        )
        own_sems = scratch[-1]

        def target_z(t):
            return lax.rem(here.z + 2 * zs - 1 - t, zs)

        def half_at(job, t, core):
            half = halves[job][1]
            return grads[job].at[
                pl.ds(target_z(t) * ys, ys), :, pl.ds(pl.multiple_of(core * half, 128), half)
            ]

        def load(job, t):
            copy = pltpu.make_async_copy(
                half_at(job, t, here.core), own[job].at[t % 2], own_sems.at[job, t % 2]
            )
            copy.start()
            return copy

        loads, by_core = {}, {}
        for wave in range(zs + max(behind)):
            for job in range(count):
                t = wave - behind[job]
                if 0 <= t < zs:
                    by_core[job, t] = copies.send(
                        half_at(job, t, lax.rem(here.core + 1, here.cores)),
                        got[job].at[t],
                        here.device(core=1),
                    )
                    if t < 2:
                        loads[job, t] = load(job, t)
        yield
        by_x, by_y, by_z = {}, {}, {}

        def base(job, t):
            return got[job].at[t] if kinds[job] == "half" else x_got[job].at[t, 0]

        def send_y(job, t):
            for turn in range(1, ys):
                by_y[job, t, turn] = copies.send(
                    base(job, t).at[lax.rem(here.y + turn, ys)],
                    y_got[job].at[t, turn - 1],
                    here.device(y=turn),
                )

        for step in range(zs + 4 + max(behind)):
            for job, kind in enumerate(kinds):
                rows, cols = shares[job]
                local = step - behind[job]
                t = local
                if 0 <= t < zs:
                    loads[job, t].wait()
                    by_core[job, t].wait_recv()
                    for y in range(ys):
                        mine, sums = own[job].at[t % 2, y], got[job].at[t, y]

                        def both(at, mine=mine, sums=sums):
                            sums[at] = (mine[at].astype(F32) + sums[at].astype(F32)).astype(BF16)

                        by_rows(halves[job][0], both)
                    if t + 2 < zs:
                        loads[job, t + 2] = load(job, t + 2)
                    if kind == "half":
                        send_y(job, t)
                    else:
                        for turn in range(1, xs):
                            x_at = lax.rem(here.x + turn, xs)
                            by_x[job, t, turn] = copies.send(
                                x_window(kind, got[job].at[t], shares[job], x_at),
                                x_got[job].at[t, turn - 1],
                                here.device(x=turn),
                            )
                t = local - 1
                if 0 <= t < zs and kind != "half":
                    for turn in range(1, xs):
                        by_x[job, t, turn].wait_recv()
                    for y in range(ys):
                        mine = x_window(kind, got[job].at[t, y], shares[job], here.x)
                        parts = [x_got[job].at[t, turn, y] for turn in range(xs - 1)]

                        def all_x(at, mine=mine, parts=parts):
                            total = mine[at].astype(F32)
                            for part in parts:
                                total += part[at].astype(F32)
                            parts[0][at] = total.astype(BF16)

                        by_rows(rows, all_x)
                    send_y(job, t)
                t = local - 2
                if 0 <= t < zs:
                    for turn in range(1, ys):
                        by_y[job, t, turn].wait_recv()
                    parts = [y_got[job].at[t, turn] for turn in range(ys - 1)]
                    target = parts[0]
                    if t > 0:
                        by_z[job, t - 1].wait_recv()
                        parts.append(z_got[job].at[t - 1])
                    if t == zs - 1:
                        target = (
                            x_sum[job].at[here.x]
                            if kind == "half"
                            else x_window(kind, done[job].at[0], shares[job], here.x)
                        )
                    mine = base(job, t).at[here.y]

                    def all_y(at, mine=mine, parts=parts, target=target):
                        total = mine[at].astype(F32)
                        for part in parts:
                            total += part[at].astype(F32)
                        target[at] = total.astype(BF16)

                    by_rows(rows, all_y)
                    if t < zs - 1:
                        by_z[job, t] = copies.send(target, z_got[job].at[t], here.device(z=1))
                    else:
                        for turn in range(1, xs):
                            by_x[job, "done", turn] = copies.send(
                                target, target, here.device(x=turn)
                            )
                if local == zs + 2:
                    for turn in range(1, xs):
                        by_x[job, "done", turn].wait_recv()
                    if kind == "half":
                        sums, target = x_sum[job], done[job].at[0]

                        def across(at, sums=sums, target=target):
                            total = sums[0, at].astype(F32)
                            for x_at in range(1, xs):
                                total += sums[x_at, at].astype(F32)
                            target[at] = total.astype(BF16)

                        by_rows(rows, across)
                    by_core[job, "done"] = copies.send(
                        done[job].at[0], done[job].at[1], here.device(core=1)
                    )
                if local == zs + 3:
                    by_core[job, "done"].wait_recv()
                    half_rows, half = halves[job]
                    if mixed[job]:
                        for core in range(2):

                            @pl.when(here.core == core)
                            def _(job=job, core=core):
                                unmix(here, done[job], outs[job], core, halves[job])

                    else:
                        for side in range(2):
                            column = lax.rem(here.core + side, 2) * half
                            place_at = outs[job].at[:, pl.ds(pl.multiple_of(column, 128), half)]

                            def write(at, place_at=place_at, source=done[job].at[side]):
                                place_at[at] = source[at].astype(F32)

                            by_rows(half_rows, write)
            yield

    return Task(
        run,
        [(value, ANY_BLOCK) for value in arrays],
        [
            (
                jax.ShapeDtypeStruct(
                    (value.shape[1], 3 * HEADS * HEAD_DIM if flag else value.shape[2]), F32
                ),
                VMEM_BLOCK,
            )
            for flag, value in zip(mixed, arrays)
        ],
        own
        + got
        + x_got
        + y_got
        + z_got
        + x_sum
        + done
        + [pltpu.SemaphoreType.DMA((count, 2))],
        copies,
    )


def lanes_of(size):
    return 128 * -(-size // 128)


def gather_vectors_task(place, narrow, wide):
    layers, small = narrow[0].shape
    large = wide.shape[1]
    count = len(narrow)
    at_large = lanes_of(small)
    lanes = at_large + lanes_of(large)
    height = 16 * -(-count * layers // 16)
    shape = (height, lanes)
    part = place.heads * HEAD_DIM
    width = small * place.shards

    def run(here, copies, ins, outs, scratch):
        rows_ref, wide_ref, bias_ref = outs
        stage, packed, landed = scratch
        stage[...] = jnp.zeros(shape, F32)
        for at, ref in enumerate(ins[:count]):
            stage[at * layers : (at + 1) * layers, :small] = ref[...].astype(F32)
        stage[0:layers, at_large : at_large + large] = ins[count][...].astype(F32)
        packed[...] = stage[...].astype(BF16)
        arriving = []
        for step in range(1, here.shards):
            to = lax.rem(here.s + step, here.shards)
            device = {"replica": here.r, "shard": to}
            arriving.append(copies.send(packed, landed.at[here.s], device))
        landed[here.s] = packed[...]
        yield
        yield
        yield
        for copy in arriving:
            copy.wait_recv()
        for s in range(here.shards):
            block = landed[s].astype(F32)
            rows_ref[:, s * small : (s + 1) * small] = block[: count * layers, :small]
            wide_ref[:, s * large : (s + 1) * large] = block[
                :layers, at_large : at_large + large
            ]
        bias_ref[...] = jnp.zeros(bias_ref.shape, F32)
        for r in range(here.replicas):
            size = min(part, width - r * part)
            if size > 0:
                for vector, place_at in ((2, 0), (3, 2)):
                    start = r * here.columns + place_at * part
                    bias_ref[:, start : start + size] = rows_ref[
                        vector * layers : (vector + 1) * layers, r * part : r * part + size
                    ]

    return Task(
        run,
        [(value, VMEM_BLOCK) for value in (*narrow, wide)],
        [
            (jax.ShapeDtypeStruct((count * layers, width), F32), VMEM_BLOCK),
            (jax.ShapeDtypeStruct((layers, large * place.shards), F32), VMEM_BLOCK),
            (jax.ShapeDtypeStruct((layers, place.replicas * place.columns), F32), VMEM_BLOCK),
        ],
        [
            pltpu.VMEM(shape, F32),
            pltpu.VMEM(shape, BF16),
            pltpu.VMEM((place.shards,) + shape, BF16),
        ],
        place.shards - 1,
    )


def reduce_vectors_task(place, by_layer):
    layers = len(by_layer)
    rows, wide, mixed = by_layer[0]
    count = len(rows)
    width, inner = rows[0].shape[1], wide.shape[1]
    small, large = width // place.shards, inner // place.shards
    at_large = lanes_of(small)
    height = 8 * -(-count * layers // 8)
    shape = (height, at_large + lanes_of(large))
    part = place.heads * HEAD_DIM
    given = [at for at, row in enumerate(rows) if row is not None]
    values = []
    for layer_rows, layer_wide, layer_mixed in by_layer:
        values += [layer_rows[at] for at in given] + [layer_wide, layer_mixed]

    def run(here, copies, ins, outs, scratch):
        (out_ref,), (lines, wides, packed, got, sums) = outs, scratch
        per = len(given) + 2
        lines[...] = jnp.zeros(lines.shape, F32)
        for layer in range(layers):
            own = ins[layer * per : (layer + 1) * per]
            for ref, at in zip(own, given):
                lines[at * layers + layer : at * layers + layer + 1, :] = ref[...]
            wides[layer : layer + 1, :] = own[-2][...]
            for r in range(here.replicas):
                size = min(part, width - r * part)
                if size > 0:
                    for vector, place_at in ((2, 0), (3, 2)):
                        row = vector * layers + layer
                        start = r * here.columns + place_at * part
                        lines[row : row + 1, r * part : r * part + size] = own[-1][
                            :, start : start + size
                        ]
        packed[...] = jnp.zeros(packed.shape, F32)
        for s in range(here.shards):
            packed[s, :, :small] = lines[:, s * small : (s + 1) * small]
            packed[s, 0:layers, at_large : at_large + large] = wides[
                :, s * large : (s + 1) * large
            ]
        arriving = []
        for step in range(1, here.shards):
            to = lax.rem(here.s + step, here.shards)
            device = {"replica": here.r, "shard": to}
            arriving.append(copies.send(packed.at[to], got.at[step - 1], device))
        yield
        yield
        yield
        for copy in arriving:
            copy.wait_recv()
        total = packed[here.s]
        for at in range(here.shards - 1):
            total += got[at]
        sums[here.r] = total
        arriving = []
        for step in range(1, here.replicas):
            device = {"replica": lax.rem(here.r + step, here.replicas), "shard": here.s}
            arriving.append(copies.send(sums.at[here.r], sums.at[here.r], device))
        yield
        yield
        for copy in arriving:
            copy.wait_recv()
        total = sums[0]
        for at in range(1, here.replicas):
            total += sums[at]
        out_ref[...] = total

    return Task(
        run,
        [(value, VMEM_BLOCK) for value in values],
        [(jax.ShapeDtypeStruct(shape, F32), VMEM_BLOCK)],
        [
            pltpu.VMEM((height, width), F32),
            pltpu.VMEM((layers, inner), F32),
            pltpu.VMEM((place.shards,) + shape, F32),
            pltpu.VMEM((place.shards - 1,) + shape, F32),
            pltpu.VMEM((place.replicas,) + shape, F32),
        ],
        place.shards + place.replicas - 2,
    )


def per_device(
    tokens,
    gain_one,
    shift_one,
    query_key_value_weight,
    b_query,
    b_value,
    output_weight,
    output_proj_bias,
    gain_two,
    shift_two,
    up_weight,
    up_bias,
    down_weight,
    down_bias,
    cotangent,
):
    place = Place(lax.axis_size("replica"), lax.axis_size("shard")).locate()
    held, _, width = tokens.shape
    layers = gain_one.shape[0]
    last = layers - 1
    mix = place.mix_columns(query_key_value_weight)
    narrow = (
        gain_one,
        shift_one,
        b_query,
        b_value,
        output_proj_bias,
        gain_two,
        shift_two,
        down_bias,
    )
    current = place.to_sequences(tokens).astype(F32)
    (first_mix,), (lines, up_lines, mix_lines) = fuse(
        place,
        "gather_first",
        0,
        [gather_task(place, [("half", mix[0])]), gather_vectors_task(place, narrow, up_bias)],
        (1, 0) * 7,
    )
    g1, s1, _, _, bo, g2, s2, bd = (
        [lines[at * layers + n : at * layers + n + 1] for n in range(layers)] for at in range(8)
    )
    mix_bias = [mix_lines[n : n + 1] for n in range(layers)]
    bu = [up_lines[n : n + 1] for n in range(layers)]
    mixes, outs = [first_mix], []
    ups, downs = [], []

    saved = []
    for n in range(layers):
        normed = norm_rows(current, g1[n], s1[n]).astype(BF16)
        mixed = (dot(normed, mixes[n], ((1,), (0,))) + mix_bias[n]).astype(BF16)
        jobs = [("columns", up_weight[n]), ("rows" if n < last else "half", down_weight[n])]
        if n == 0:
            jobs.append(("half", output_weight[0]))
        if n < last:
            jobs += [("half", mix[n + 1]), ("half", output_weight[n + 1])]
        (seq, attended), gathered = fuse(
            place,
            f"attend_{n}",
            1 + n,
            [attend_task(place, mixed), gather_task(place, jobs)],
            (0, 1, 1, 0) + (0, 1) * place.replicas,
        )
        ups.append(gathered.pop(0))
        downs.append(gathered.pop(0))
        if n == 0:
            outs.append(gathered.pop(0))
        if n < last:
            mixes.append(gathered.pop(0))
            outs.append(gathered.pop(0))
        x_mid = current + (dot(attended, outs[n], ((1,), (0,))) + bo[n])
        moved = norm_rows(x_mid, g2[n], s2[n]).astype(BF16)
        pre = dot(moved, ups[n], ((1,), (0,))) + bu[n]
        act = jax.nn.gelu(pre, approximate=True).astype(BF16)
        saved.append((current, normed, seq, attended, x_mid, moved, pre, act))
        current = x_mid + dot(act, downs[n], ((1,), (0,))) + bd[n]
    output = place.from_sequences(current.astype(BF16), held)

    grad_now = place.to_sequences(cotangent).astype(F32)
    summed = [{} for _ in range(layers)]
    vector_grads = [None] * layers
    waiting = []
    for n in reversed(range(layers)):
        current, normed, seq, attended, x_mid, moved, pre, act = saved[n]
        d_ffn = grad_now.astype(BF16)
        grad_down = dot(act, d_ffn, ((0,), (0,))).astype(BF16)
        grad_b_down = jnp.sum(d_ffn.astype(F32), 0, keepdims=True)
        d_act = dot(d_ffn, downs[n], ((1,), (1,)))
        gelu_back = jax.vjp(lambda inner: jax.nn.gelu(inner, approximate=True), pre)[1]
        d_pre = gelu_back(d_act)[0].astype(BF16)
        grad_up = dot(moved, d_pre, ((0,), (0,))).astype(BF16)
        grad_b_up = jnp.sum(d_pre.astype(F32), 0, keepdims=True)
        d_moved = dot(d_pre, ups[n], ((1,), (1,)))
        d_from_norm, grad_gain_two, grad_shift_two = norm_rows_back(x_mid, g2[n], d_moved)
        grad_mid = grad_now + d_from_norm
        d_branch = grad_mid.astype(BF16)
        grad_out = dot(attended, d_branch, ((0,), (0,))).astype(BF16)
        grad_b_out = jnp.sum(d_branch.astype(F32), 0, keepdims=True)
        d_att = dot(d_branch, outs[n], ((1,), (1,))).astype(BF16)
        waiting += [("up", n, "columns", False, grad_up), ("down", n, "half", False, grad_down)]
        (d_mixed,), sums = fuse(
            place,
            f"attend_back_{n}",
            1 + layers + n,
            [
                attend_back_task(place, seq, d_att),
                reduce_task(place, [job[2:] for job in waiting]),
            ],
            (0, 1, 1, 0) + (0, 1) * place.replicas,
        )
        for job, value in zip(waiting, sums):
            summed[job[1]][job[0]] = value
        grad_mix = dot(normed, d_mixed, ((0,), (0,))).astype(BF16)
        waiting = [("mix", n, "half", True, grad_mix), ("out", n, "half", False, grad_out)]
        grad_b_mix = jnp.sum(d_mixed.astype(F32), 0, keepdims=True)
        d_normed = dot(d_mixed, mixes[n], ((1,), (1,)))
        d_from_first, grad_gain_one, grad_shift_one = norm_rows_back(current, g1[n], d_normed)
        grad_now = grad_mid + d_from_first
        vector_grads[n] = (
            (
                grad_gain_one,
                grad_shift_one,
                None,
                None,
                grad_b_out,
                grad_gain_two,
                grad_shift_two,
                grad_b_down,
            ),
            grad_b_up,
            grad_b_mix,
        )
    grad_tokens = place.from_sequences(grad_now.astype(BF16), held).astype(F32)
    sums, (vector_sums,) = fuse(
        place,
        "reduce_last",
        1 + 2 * layers,
        [
            reduce_task(place, [job[2:] for job in waiting]),
            reduce_vectors_task(place, vector_grads),
        ],
        (1, 0) * 8,
    )
    for job, value in zip(waiting, sums):
        summed[job[1]][job[0]] = value
    weight_grads = {
        name: jnp.stack([summed[n][name] for n in range(layers)])
        for name in ("mix", "out", "up", "down")
    }
    small = gain_one.shape[1]
    (
        grad_gain_one,
        grad_shift_one,
        grad_b_query,
        grad_b_value,
        grad_b_out,
        grad_gain_two,
        grad_shift_two,
        grad_b_down,
    ) = (vector_sums[at * layers : (at + 1) * layers, :small] for at in range(8))
    start = lanes_of(small)
    grad_b_up = vector_sums[:layers, start : start + up_bias.shape[1]]
    return (
        output,
        grad_tokens,
        grad_gain_one,
        grad_shift_one,
        weight_grads["mix"],
        grad_b_query,
        grad_b_value,
        weight_grads["out"],
        grad_b_out,
        grad_gain_two,
        grad_shift_two,
        weight_grads["up"],
        grad_b_up,
        weight_grads["down"],
        grad_b_down,
    )


def solution(mesh):
    vector, matrix = P(None, "shard"), P(None, "shard", None)
    rows = P("replica", "shard", None)
    in_specs = (
        rows,
        vector,
        vector,
        matrix,
        vector,
        vector,
        matrix,
        vector,
        vector,
        vector,
        matrix,
        vector,
        matrix,
        vector,
        rows,
    )
    out_specs = (
        rows,
        rows,
        vector,
        vector,
        matrix,
        vector,
        vector,
        matrix,
        vector,
        vector,
        vector,
        matrix,
        vector,
        matrix,
        vector,
    )
    return jax.shard_map(
        per_device, mesh=mesh, in_specs=in_specs, out_specs=out_specs, check_vma=False
    )
```
